32 devices in a mesh: rep: 1 (over z), heads: 4 (over y), pool: 8 (over x, core).
Axes of the slice: x: 4, y: 4, z: 1, core: 2. Of those that a mesh axis runs over, the one named last changes fastest.
The devices are a block of a 4x4x8 slice.
Arguments:
- kv_pool: bfloat16 [1, 128, 2, 128, 32, 128], P(None, ('rep', 'pool'), None, None, 'heads')
- page_idx: int32 [8, 8, 1], P('rep', 'pool')
- x_tokens: bfloat16 [8, 512, 4096], P(('rep', 'pool'))
- gain_attn: bfloat16 [1, 4096], replicated
- w_q: bfloat16 [1, 4096, 4096], P(None, None, 'heads')
- w_k: bfloat16 [1, 4096, 4096], P(None, None, 'heads')
- w_v: bfloat16 [1, 4096, 4096], P(None, None, 'heads')
- w_o: bfloat16 [1, 4096, 4096], P(None, 'heads')
- gain_mlp: bfloat16 [1, 4096], replicated
- w_gate: bfloat16 [1, 4096, 11008], P(None, None, 'heads')
- w_up: bfloat16 [1, 4096, 11008], P(None, None, 'heads')
- w_down: bfloat16 [1, 11008, 4096], P(None, 'heads')
Outputs:
- output: bfloat16 [8, 512, 4096], P(('rep', 'pool'))
All inputs are finite; a program needn't handle non-finite values.
Results may differ from the reference program's by a relative error of at most 0.0130825.
Values are sent between devices in bfloat16 or wider.
A program may use at most 768 MiB of HBM per device.

```python
import jax
import jax.numpy as jnp
from jax import lax

LAYERS = 1
OWNERS = 8
POOL_PAGES = 16
REQ_PAGES = 1
PAGE_LEN = 128
KV_HEADS = 32
HEAD_DIM = 128
TOKENS = 512
D_MODEL = 4096
Q_HEADS = 32
FFN_DIM = 11008

PREFIX = OWNERS * REQ_PAGES * PAGE_LEN
GROUP_Q = Q_HEADS // KV_HEADS


def setup_inputs(seed: int = 0, part: int = 0) -> dict:
    shared_keys = jax.random.split(jax.random.key(seed), 10)
    part_keys = jax.random.split(jax.random.fold_in(jax.random.key(seed + 1), part), 3)
    pool_shape = (LAYERS, OWNERS * POOL_PAGES, 2, PAGE_LEN, KV_HEADS, HEAD_DIM)
    kv_pool = (2.0 * jax.random.normal(part_keys[0], pool_shape, jnp.float32)).astype(jnp.bfloat16)
    pick_keys = jax.random.split(part_keys[1], OWNERS * OWNERS)
    page_idx = jax.vmap(lambda one_key: jax.random.permutation(one_key, POOL_PAGES)[:REQ_PAGES])(pick_keys)
    page_idx = page_idx.reshape(OWNERS, OWNERS, REQ_PAGES).astype(jnp.int32)
    x_tokens = (0.5 * jax.random.normal(part_keys[2], (OWNERS, TOKENS, D_MODEL), jnp.float32)).astype(jnp.bfloat16)

    def draw_weight(w_key, arr_shape, fan_in):
        return (jax.random.normal(w_key, arr_shape, jnp.float32) * fan_in ** -0.5).astype(jnp.bfloat16)

    def draw_gains(g_key):
        return (1.0 + 0.3 * jax.random.normal(g_key, (LAYERS, D_MODEL), jnp.float32)).astype(jnp.bfloat16)

    q_width = Q_HEADS * HEAD_DIM
    kv_width = KV_HEADS * HEAD_DIM
    return {
        'kv_pool': kv_pool,
        'page_idx': page_idx,
        'x_tokens': x_tokens,
        'gain_attn': draw_gains(shared_keys[0]),
        'w_q': draw_weight(shared_keys[1], (LAYERS, D_MODEL, q_width), D_MODEL),
        'w_k': draw_weight(shared_keys[2], (LAYERS, D_MODEL, kv_width), D_MODEL / 4.0),
        'w_v': draw_weight(shared_keys[3], (LAYERS, D_MODEL, kv_width), D_MODEL / 4.0),
        'w_o': draw_weight(shared_keys[4], (LAYERS, q_width, D_MODEL), q_width),
        'gain_mlp': draw_gains(shared_keys[5]),
        'w_gate': draw_weight(shared_keys[6], (LAYERS, D_MODEL, FFN_DIM), D_MODEL),
        'w_up': draw_weight(shared_keys[7], (LAYERS, D_MODEL, FFN_DIM), D_MODEL),
        'w_down': draw_weight(shared_keys[8], (LAYERS, FFN_DIM, D_MODEL), FFN_DIM),
    }


def rms_norm(hidden, gain_vec):
    hid_f32 = hidden.astype(jnp.float32)
    inv_rms = lax.rsqrt(jnp.mean(hid_f32 * hid_f32, axis=-1, keepdims=True) + 1e-5)
    return (hid_f32 * inv_rms * gain_vec.astype(jnp.float32)).astype(jnp.bfloat16)


def rope_tables():
    positions = (PREFIX + jnp.arange(TOKENS)).astype(jnp.float32)
    inv_freq = 10000.0 ** (-2.0 * jnp.arange(HEAD_DIM // 2).astype(jnp.float32) / HEAD_DIM)
    angles = positions[:, None] * inv_freq[None, :]
    return jnp.cos(angles)[:, None, :], jnp.sin(angles)[:, None, :]


def apply_rope(projected, cos_tab, sin_tab):
    half_dim = HEAD_DIM // 2
    first_half = projected[..., :half_dim]
    second_half = projected[..., half_dim:]
    return jnp.concatenate([first_half * cos_tab - second_half * sin_tab, second_half * cos_tab + first_half * sin_tab], axis=-1)


def reference(kv_pool, page_idx, x_tokens, gain_attn, w_q, w_k, w_v, w_o, gain_mlp, w_gate, w_up, w_down):
    cos_tab, sin_tab = rope_tables()
    owner_base = jnp.arange(OWNERS)[:, None] * POOL_PAGES
    allowed = jnp.arange(PREFIX + TOKENS)[None, :] <= PREFIX + jnp.arange(TOKENS)[:, None]

    def layer_step(hidden, layer_in):
        pool_layer, gain_a, wq_layer, wk_layer, wv_layer, wo_layer, gain_m, wg_layer, wu_layer, wd_layer = layer_in
        h_att = rms_norm(hidden, gain_a).reshape(OWNERS * TOKENS, D_MODEL)
        q_proj = jnp.dot(h_att, wq_layer, preferred_element_type=jnp.float32).reshape(OWNERS, TOKENS, Q_HEADS, HEAD_DIM)
        k_proj = jnp.dot(h_att, wk_layer, preferred_element_type=jnp.float32).reshape(OWNERS, TOKENS, KV_HEADS, HEAD_DIM)
        queries = apply_rope(q_proj, cos_tab, sin_tab).astype(jnp.bfloat16)
        k_new = apply_rope(k_proj, cos_tab, sin_tab).astype(jnp.bfloat16)
        v_new = jnp.dot(h_att, wv_layer, preferred_element_type=jnp.float32).astype(jnp.bfloat16).reshape(OWNERS, TOKENS, KV_HEADS, HEAD_DIM)

        def one_request(per_req):
            q_req, k_req, v_req, idx_req = per_req
            page_rows = (owner_base + idx_req).reshape(OWNERS * REQ_PAGES)
            fetched = pool_layer[page_rows]
            key_all = jnp.concatenate([fetched[:, 0].reshape(PREFIX, KV_HEADS, HEAD_DIM), k_req], axis=0).astype(jnp.float32)
            val_all = jnp.concatenate([fetched[:, 1].reshape(PREFIX, KV_HEADS, HEAD_DIM), v_req], axis=0).astype(jnp.float32)
            q_grp = q_req.astype(jnp.float32).reshape(TOKENS, KV_HEADS, GROUP_Q, HEAD_DIM)
            scores = jnp.einsum('tgrd,ngd->grtn', q_grp, key_all) * HEAD_DIM ** -0.5
            scores = jnp.where(allowed, scores, -jnp.inf)
            probs_bf = jax.nn.softmax(scores, axis=-1).astype(jnp.bfloat16)
            attn_sum = jnp.einsum('grtn,ngd->tgrd', probs_bf.astype(jnp.float32), val_all)
            return attn_sum.reshape(TOKENS, Q_HEADS * HEAD_DIM).astype(jnp.bfloat16)

        attn_cat = lax.map(one_request, (queries, k_new, v_new, page_idx))
        attn_out = jnp.dot(attn_cat.reshape(OWNERS * TOKENS, Q_HEADS * HEAD_DIM), wo_layer, preferred_element_type=jnp.float32).reshape(OWNERS, TOKENS, D_MODEL)
        x_mid = (hidden.astype(jnp.float32) + attn_out).astype(jnp.bfloat16)
        h_mlp = rms_norm(x_mid, gain_m).reshape(OWNERS * TOKENS, D_MODEL)
        gate_proj = jnp.dot(h_mlp, wg_layer, preferred_element_type=jnp.float32)
        up_proj = jnp.dot(h_mlp, wu_layer, preferred_element_type=jnp.float32)
        act_out = (jax.nn.silu(gate_proj) * up_proj).astype(jnp.bfloat16)
        mlp_out = jnp.dot(act_out, wd_layer, preferred_element_type=jnp.float32).reshape(OWNERS, TOKENS, D_MODEL)
        return (x_mid.astype(jnp.float32) + mlp_out).astype(jnp.bfloat16), None

    x_out, _ = lax.scan(layer_step, x_tokens, (kv_pool, gain_attn, w_q, w_k, w_v, w_o, gain_mlp, w_gate, w_up, w_down))
    return x_out
```

```python
import functools

import jax
import jax.numpy as jnp
from jax import lax
from jax.experimental import pallas as pl
from jax.experimental.pallas import tpu as pltpu
from jax.sharding import PartitionSpec as P

MESH = pl.DeviceIdType.MESH
BF16 = jnp.bfloat16
F32 = jnp.float32
ANY = pl.BlockSpec(memory_space=pl.ANY)
VMEM_MAX = 67043328


def rms_norm(hidden, gain_vec):
    hid_f32 = hidden.astype(F32)
    inv_rms = lax.rsqrt(jnp.mean(hid_f32 * hid_f32, axis=-1, keepdims=True) + 1e-5)
    return (hid_f32 * inv_rms * gain_vec.astype(F32)).astype(BF16)


def rope_tables(prefix, tokens, head_dim):
    positions = (prefix + jnp.arange(tokens)).astype(F32)
    inv_freq = 10000.0 ** (-2.0 * jnp.arange(head_dim // 2).astype(F32) / head_dim)
    angles = positions[:, None] * inv_freq[None, :]
    cos_half, sin_half = jnp.cos(angles), jnp.sin(angles)
    return jnp.concatenate([cos_half, cos_half], axis=-1), jnp.concatenate([-sin_half, sin_half], axis=-1)


def ring_neighbours(axis, size):
    me = lax.axis_index(axis)
    return me, lax.rem(me + 1, size), lax.rem(me + size - 1, size)


def greet(left, right):
    barrier = pltpu.get_barrier_semaphore()
    for neighbour in (left, right):
        pl.semaphore_signal(barrier, inc=1, device_id={"heads": neighbour}, device_id_type=MESH)
    pl.semaphore_wait(barrier, 2)


def remote(src, dst, send_sem, recv_sem, target):
    return pltpu.make_async_remote_copy(
        src_ref=src, dst_ref=dst, send_sem=send_sem, recv_sem=recv_sem, device_id={"heads": target}, device_id_type=MESH
    )


def attend_kernel(ring, head_dim, heads, q_ref, k_ref, v_ref, kv_ref, cos_ref, sin_ref, out_ref, gathered, send_sem, recv_sem, out_sem):
    me, right, left = ring_neighbours("heads", ring)
    tokens = q_ref.shape[0]
    half = tokens // 2
    prefix = kv_ref.shape[0] * kv_ref.shape[3]
    scale = head_dim ** -0.5
    nt = (((1,), (1,)), ((), ()))
    greet(left, right)

    def lanes(g):
        return pl.ds(pl.multiple_of(g * head_dim, head_dim), head_dim)

    def direct(g, way):
        piece = gathered.at[me, :, lanes(g)]
        return remote(piece, piece, send_sem.at[g, 0, way], recv_sem.at[g, 0, way], (right, left)[way])

    def passed(g, way):
        rows = pl.ds(way * half, half)
        piece = gathered.at[(left, right)[way], rows, lanes(g)]
        return remote(piece, piece, send_sem.at[g, 1, way], recv_sem.at[g, 1, way], (right, left)[way])

    def forward(g):
        for way in range(2):
            direct(g, way).wait_recv()
            passed(g, way).start()

    def rope(ref, g):
        val = ref[:, lanes(g)]
        return (val * cos_ref[...] + pltpu.roll(val, head_dim // 2, 1) * sin_ref[...]).astype(BF16)

    def one_head(g, carry):
        queries, keys_new = rope(q_ref, g), rope(k_ref, g)
        keys_pre = kv_ref[:, g, 0].reshape(prefix, head_dim)
        vals_pre = kv_ref[:, g, 1].reshape(prefix, head_dim)
        vals_new = v_ref[:, lanes(g)]
        for part in range(2):
            rows = slice(part * half, (part + 1) * half)
            seen = (part + 1) * half
            q_part = queries[rows]
            s_pre = lax.dot_general(q_part, keys_pre, nt, preferred_element_type=F32) * scale
            s_new = lax.dot_general(q_part, keys_new[:seen], nt, preferred_element_type=F32) * scale
            t_id = lax.broadcasted_iota(jnp.int32, s_new.shape, 0) + part * half
            u_id = lax.broadcasted_iota(jnp.int32, s_new.shape, 1)
            s_new = jnp.where(t_id >= u_id, s_new, -jnp.inf)
            row_max = jnp.maximum(jnp.max(s_pre, axis=-1, keepdims=True), jnp.max(s_new, axis=-1, keepdims=True))
            e_pre = jnp.exp(s_pre - row_max)
            e_new = jnp.exp(s_new - row_max)
            inv_den = 1.0 / (jnp.sum(e_pre, axis=-1, keepdims=True) + jnp.sum(e_new, axis=-1, keepdims=True))
            total = jnp.dot((e_pre * inv_den).astype(BF16), vals_pre, preferred_element_type=F32)
            total = total + jnp.dot((e_new * inv_den).astype(BF16), vals_new[:seen], preferred_element_type=F32)
            gathered[me, rows, lanes(g)] = total.astype(BF16)
        for way in range(2):
            direct(g, way).start()

        @pl.when(g > 0)
        def _():
            forward(g - 1)

        return carry

    lax.fori_loop(0, heads, one_head, 0)
    forward(heads - 1)

    def settle(g, carry):
        for way in range(2):
            direct(g, way).wait_send()
            passed(g, way).wait()
        return carry

    lax.fori_loop(0, heads, settle, 0)
    copy = pltpu.make_async_copy(gathered, out_ref, out_sem)
    copy.start()
    copy.wait()


def attend(call_id, ring, part, heads, head_dim, q, k, v, kv, cos_tab, sin_tab):
    tokens = q.shape[0]
    width = heads * head_dim
    cols = pl.BlockSpec((tokens, width), lambda i: (0, part))
    whole = lambda arr: pl.BlockSpec(arr.shape, lambda i: (0,) * arr.ndim)
    keys = kv.shape[0] * kv.shape[3] + tokens
    return pl.pallas_call(
        functools.partial(attend_kernel, ring, head_dim, heads),
        grid=(1,),
        out_shape=jax.ShapeDtypeStruct((ring, tokens, width), BF16),
        in_specs=[cols, cols, cols, whole(kv), whole(cos_tab), whole(sin_tab)],
        out_specs=ANY,
        scratch_shapes=[
            pltpu.VMEM((ring, tokens, width), BF16),
            pltpu.SemaphoreType.DMA((heads, 2, 2)),
            pltpu.SemaphoreType.DMA((heads, 2, 2)),
            pltpu.SemaphoreType.DMA,
        ],
        compiler_params=pltpu.CompilerParams(collective_id=call_id, has_side_effects=True, vmem_limit_bytes=48 * 2**20),
        cost_estimate=pl.CostEstimate(flops=16 * width * tokens * keys, bytes_accessed=8 * 2**20, transcendentals=heads * tokens * keys),
        name=f"attend_{part}",
    )(q, k, v, kv, cos_tab, sin_tab)


CHUNKS = 2
GROUPS = 4
K_BLOCK = 512


def mlp_kernel(ring, core, a0_ref, a1_ref, wm_ref, wo_ref, x_ref, gain_ref, wg_ref, wu_ref, wd_ref, out_ref,
               mid, normed, gate_w, up_w, part_sum, running, result,
               local_sem, w_sem, d_sem, mid_send, mid_recv, rs_send, rs_recv, ag_send, ag_recv, out_sem):
    me, right, left = ring_neighbours("heads", ring)
    ways = (right, left)
    half_id = core()
    tokens, width = x_ref.shape
    block = width // ring
    hid = wg_ref.shape[1]
    rows_c = tokens // CHUNKS
    rows_g = tokens // GROUPS
    per_chunk = GROUPS // CHUNKS
    k_steps = width // K_BLOCK
    n_half = block // 2
    a_cols = a0_ref.shape[2]

    def load_gate_up(kk):
        rows = pl.ds(pl.multiple_of(lax.rem(kk, k_steps) * K_BLOCK, K_BLOCK), K_BLOCK)
        slot = lax.rem(kk, 2)
        return (pltpu.make_async_copy(wg_ref.at[rows], gate_w.at[slot], w_sem.at[0, slot]),
                pltpu.make_async_copy(wu_ref.at[rows], up_w.at[slot], w_sem.at[1, slot]))

    for copy in load_gate_up(0):
        copy.start()

    greet(left, right)

    def mid_direct(c, way):
        piece = mid.at[me, pl.ds(c * rows_c, rows_c)]
        return remote(piece, piece, mid_send.at[c, 0, way], mid_recv.at[c, 0, way], ways[way])

    def mid_passed(c, way):
        piece = mid.at[(left, right)[way], pl.ds(c * rows_c + way * (rows_c // 2), rows_c // 2)]
        return remote(piece, piece, mid_send.at[c, 1, way], mid_recv.at[c, 1, way], ways[way])

    def mid_forward(c):
        for way in range(2):
            mid_direct(c, way).wait_recv()
            mid_passed(c, way).start()

    def output_product(a_buf, w_buf, x_buf):
        copies = [
            pltpu.make_async_copy(a0_ref, a_buf.at[0], local_sem.at[0]),
            pltpu.make_async_copy(a1_ref, a_buf.at[1], local_sem.at[1]),
            pltpu.make_async_copy(wm_ref, w_buf.at[half_id], local_sem.at[2]),
            pltpu.make_async_copy(wo_ref, w_buf.at[1 - half_id], local_sem.at[3]),
            pltpu.make_async_copy(x_ref.at[:, pl.ds(pl.multiple_of(me * block, block), block)], x_buf, local_sem.at[4]),
        ]
        for copy in copies:
            copy.start()
        for copy in copies:
            copy.wait()
        for c in range(CHUNKS):
            for n in range(2):
                cols = slice(n * n_half, (n + 1) * n_half)
                rows = slice(c * rows_c, (c + 1) * rows_c)
                total = jnp.zeros((rows_c, n_half), F32)
                for hf in range(2):
                    for src in range(ring):
                        total = total + jnp.dot(a_buf[hf, src, rows], w_buf[hf, src, :, cols], preferred_element_type=F32)
                mid[me, rows, cols] = (x_buf[rows, cols].astype(F32) + total).astype(BF16)
            if c > 0:
                mid_forward(c - 1)
            for way in range(2):
                mid_direct(c, way).start()

    pl.run_scoped(
        output_product,
        pltpu.VMEM((2, ring, tokens, a_cols), BF16),
        pltpu.VMEM((2, ring, a_cols, block), BF16),
        pltpu.VMEM((tokens, block), BF16),
    )

    def mid_settle(c):
        for way in range(2):
            mid_passed(c, way).wait_recv()

    def rs_block(s, way):
        return lax.rem(me + ring - 1 - s, ring) if way == 0 else lax.rem(me + 1 + s, ring)

    def rs_send_copy(r, s, way):
        rows = pl.ds((r % per_chunk) * rows_g, rows_g)
        src = part_sum.at[r // per_chunk, 0, way, rows] if s == 0 else running.at[r, s - 1, way]
        return remote(src, running.at[r, s, way], rs_send.at[r, s, way], rs_recv.at[r, s, way], ways[way])

    def rs_step(r, s):
        rows = slice((r % per_chunk) * rows_g, (r % per_chunk + 1) * rows_g)
        for way in range(2):
            rs_send_copy(r, s - 1, way).wait_recv()
            running[r, s - 1, way] = running[r, s - 1, way] + part_sum[r // per_chunk, s, way, rows]
            rs_send_copy(r, s, way).start()

    def ag_direct(r, way):
        piece = result.at[me, pl.ds(r * rows_g, rows_g)]
        return remote(piece, piece, ag_send.at[r, 0, way], ag_recv.at[r, 0, way], ways[way])

    def ag_passed(r, way):
        piece = result.at[(left, right)[way], pl.ds(r * rows_g + way * (rows_g // 2), rows_g // 2)]
        return remote(piece, piece, ag_send.at[r, 1, way], ag_recv.at[r, 1, way], ways[way])

    def rs_final(r):
        rows = slice((r % per_chunk) * rows_g, (r % per_chunk + 1) * rows_g)
        dst = slice(r * rows_g, (r + 1) * rows_g)
        for way in range(2):
            rs_send_copy(r, ring - 2, way).wait_recv()
            cols = slice(way * n_half, (way + 1) * n_half)
            total = running[r, ring - 2, way] + part_sum[r // per_chunk, ring - 1, way, rows]
            result[me, dst, cols] = (mid[me, dst, cols].astype(F32) + total).astype(BF16)
        for way in range(2):
            ag_direct(r, way).start()

    def ag_forward(r):
        for way in range(2):
            ag_direct(r, way).wait_recv()
            ag_passed(r, way).start()

    def put_out(r, src):
        rows = pl.ds(r * rows_g, rows_g)
        cols = pl.ds(src * block, block)
        return pltpu.make_async_copy(result.at[src, rows], out_ref.at[rows, cols], out_sem.at[r, src])

    def ag_settle(r):
        for way in range(2):
            ag_passed(r, way).wait_recv()
        for src in range(ring):
            put_out(r, src).start()

    def hidden_part(acc_g, acc_u, act, down_w, gain_buf):
        gain_copy = pltpu.make_async_copy(gain_ref, gain_buf, local_sem.at[0])
        gain_copy.start()
        gain_copy.wait()

        def load_down(jj):
            s, way = lax.rem(jj // 2, ring), lax.rem(jj, 2)
            blk = jnp.where(way == 0, lax.rem(me + 2 * ring - 1 - s, ring), lax.rem(me + 1 + s, ring))
            col = pl.multiple_of(blk * block + way * n_half, n_half)
            slot = lax.rem(jj, 3)
            return pltpu.make_async_copy(wd_ref.at[:, pl.ds(col, n_half)], down_w.at[slot], d_sem.at[slot])

        for jj in range(2):
            load_down(jj).start()

        def normalise(c):
            for sub in range(rows_c // 128):
                rows = slice(c * rows_c + sub * 128, c * rows_c + (sub + 1) * 128)
                squares = jnp.zeros((128, 1), F32)
                for b in range(ring):
                    val = mid[b, rows].astype(F32)
                    squares = squares + jnp.sum(val * val, axis=-1, keepdims=True)
                inv_rms = lax.rsqrt(squares * (1.0 / width) + 1e-5)
                for b in range(ring):
                    gain = gain_buf[:, b * block:(b + 1) * block].astype(F32)
                    normed[b, sub * 128:(sub + 1) * 128] = (mid[b, rows].astype(F32) * inv_rms * gain).astype(BF16)

        def gate_up(c, tasks):
            acc_g[...] = jnp.zeros(acc_g.shape, F32)
            acc_u[...] = jnp.zeros(acc_u.shape, F32)
            per_block = block // K_BLOCK

            def body(kb, carry):
                kk = c * k_steps + kb
                slot = lax.rem(kk, 2)
                loaded = load_gate_up(kk)
                for copy in loaded:
                    copy.wait()

                @pl.when(kk + 1 < CHUNKS * k_steps)
                def _():
                    for copy in load_gate_up(kk + 1):
                        copy.start()

                lhs = normed[kb // per_block, :, pl.ds(pl.multiple_of(lax.rem(kb, per_block) * K_BLOCK, K_BLOCK), K_BLOCK)]
                acc_g[...] += jnp.dot(lhs, gate_w[slot], preferred_element_type=F32)
                acc_u[...] += jnp.dot(lhs, up_w[slot], preferred_element_type=F32)
                for at, task in tasks:
                    pl.when(kb == at)(task)
                return carry

            lax.fori_loop(0, k_steps, body, 0)
            for sub in range(rows_c // 32):
                rows = slice(sub * 32, (sub + 1) * 32)
                gate = acc_g[rows]
                act[rows] = (gate * jax.nn.sigmoid(gate) * acc_u[rows]).astype(BF16)

        def down(c, tasks):
            def body(s, carry):
                for way in range(2):
                    jj = c * 2 * ring + 2 * s + way
                    load_down(jj).wait()

                    @pl.when(jj + 2 < CHUNKS * 2 * ring)
                    def _():
                        load_down(jj + 2).start()

                    part_sum[c, s, way] = jnp.dot(act[...], down_w[lax.rem(jj, 3)], preferred_element_type=F32)

                @pl.when(s == 0)
                def _():
                    for sub in range(per_chunk):
                        for way in range(2):
                            rs_send_copy(c * per_chunk + sub, 0, way).start()

                for at, task in tasks:
                    pl.when(s == at)(task)
                return carry

            lax.fori_loop(0, ring, body, 0)

        do = functools.partial
        mid_settle(0)
        normalise(0)
        gate_up(0, [(4, do(mid_forward, 1))])
        down(0, [])
        mid_settle(1)
        normalise(1)
        gate_up(1, [(1, do(rs_step, 0, 1)), (3, do(rs_step, 1, 1)), (5, do(rs_step, 0, 2)), (7, do(rs_step, 1, 2))])
        down(1, [(1, do(rs_final, 0)), (3, do(rs_final, 1))])

    pl.run_scoped(
        hidden_part,
        pltpu.VMEM((rows_c, hid), F32),
        pltpu.VMEM((rows_c, hid), F32),
        pltpu.VMEM((rows_c, hid), BF16),
        pltpu.VMEM((3, hid, n_half), BF16),
        pltpu.VMEM((1, width), BF16),
    )

    rs_step(2, 1)
    rs_step(3, 1)
    ag_forward(0)
    rs_step(2, 2)
    ag_forward(1)
    rs_step(3, 2)
    rs_final(2)
    rs_final(3)
    ag_settle(0)
    ag_settle(1)
    ag_forward(2)
    ag_forward(3)
    ag_settle(2)
    ag_settle(3)
    for c in range(CHUNKS):
        for way in range(2):
            mid_direct(c, way).wait_send()
            mid_passed(c, way).wait_send()
    for r in range(GROUPS):
        for way in range(2):
            for s in range(ring - 1):
                rs_send_copy(r, s, way).wait_send()
            ag_direct(r, way).wait_send()
            ag_passed(r, way).wait_send()
        for src in range(ring):
            put_out(r, src).wait()


def mlp(call_id, ring, core, a0, a1, w_mine, w_other, x, gain, w_gate, w_up, w_down):
    tokens, width = x.shape
    hid = w_gate.shape[1]
    block = width // ring
    rows_c, rows_g = tokens // CHUNKS, tokens // GROUPS
    dma = pltpu.SemaphoreType.DMA
    return pl.pallas_call(
        functools.partial(mlp_kernel, ring, core),
        out_shape=jax.ShapeDtypeStruct((tokens, width), BF16),
        in_specs=[ANY] * 9,
        out_specs=ANY,
        scratch_shapes=[
            pltpu.VMEM((ring, tokens, block), BF16),
            pltpu.VMEM((ring, rows_c, block), BF16),
            pltpu.VMEM((2, K_BLOCK, hid), BF16),
            pltpu.VMEM((2, K_BLOCK, hid), BF16),
            pltpu.VMEM((CHUNKS, ring, 2, rows_c, block // 2), F32),
            pltpu.VMEM((GROUPS, ring - 1, 2, rows_g, block // 2), F32),
            pltpu.VMEM((ring, tokens, block), BF16),
            dma((5,)), dma((2, 2)), dma((3,)),
            dma((CHUNKS, 2, 2)), dma((CHUNKS, 2, 2)),
            dma((GROUPS, ring - 1, 2)), dma((GROUPS, ring - 1, 2)),
            dma((GROUPS, 2, 2)), dma((GROUPS, 2, 2)),
            dma((GROUPS, ring)),
        ],
        compiler_params=pltpu.CompilerParams(collective_id=call_id, has_side_effects=True, vmem_limit_bytes=VMEM_MAX),
        cost_estimate=pl.CostEstimate(flops=2 * tokens * width * (block + 3 * hid), bytes_accessed=160 * 2**20, transcendentals=tokens * hid),
        name="mlp",
    )(a0, a1, w_mine, w_other, x, gain, w_gate, w_up, w_down)


def solution(mesh):
    owners = mesh.shape["pool"]
    ring = mesh.shape["heads"]
    assert ring == 4 and owners % 2 == 0

    def local_fn(kv_pool, page_idx, x_tokens, gain_attn, w_q, w_k, w_v, w_o, gain_mlp, w_gate, w_up, w_down):
        layers, _, _, page_len, kv_loc, head_dim = kv_pool.shape
        tokens, width = x_tokens.shape[1:]
        req_pages = page_idx.shape[2]
        prefix = owners * req_pages * page_len
        wanted = page_idx.reshape(owners * req_pages)
        cos_tab, sin_tab = rope_tables(prefix, tokens, head_dim)
        core = lambda: lax.rem(lax.axis_index("pool"), 2)
        swap = [(i, i ^ 1) for i in range(owners)]
        hidden = x_tokens[0]
        heads = kv_loc // 2
        for layer in range(layers):
            picked = kv_pool.at[layer, wanted].get(mode="promise_in_bounds").transpose(0, 3, 1, 2, 4)
            rows_half = w_o.shape[1] // 2
            mine = lax.dynamic_slice_in_dim(w_o[layer], core() * rows_half, rows_half, 0)
            mine = mine.reshape(rows_half, ring, width // ring).transpose(1, 0, 2)
            received = [lax.all_to_all(picked[:, p * heads:(p + 1) * heads], "pool", 0, 0, tiled=True) for p in range(2)]
            wo_mine = lax.all_to_all(mine, "heads", 0, 0, tiled=True)
            wo_other = lax.ppermute(wo_mine, "pool", swap)
            h_att = rms_norm(hidden, gain_attn[layer])
            q = jnp.dot(h_att, w_q[layer], preferred_element_type=F32)
            k = jnp.dot(h_att, w_k[layer], preferred_element_type=F32)
            v = jnp.dot(h_att, w_v[layer], preferred_element_type=F32).astype(BF16)
            a0, a1 = (attend(3 * layer + p, ring, p, heads, head_dim, q, k, v, received[p], cos_tab, sin_tab) for p in range(2))
            hidden = mlp(3 * layer + 2, ring, core, a0, a1, wo_mine, wo_other, hidden, gain_mlp[layer][None], w_gate[layer], w_up[layer], w_down[layer])
        return hidden[None]

    pool_spec = P(None, ("rep", "pool"), None, None, "heads", None)
    index_spec = P("rep", "pool", None)
    x_spec = P(("rep", "pool"), None, None)
    gain_spec = P(None, None)
    col_spec = P(None, None, "heads")
    row_spec = P(None, "heads", None)
    return jax.shard_map(local_fn, mesh=mesh, in_specs=(pool_spec, index_spec, x_spec, gain_spec, col_spec, col_spec, col_spec, row_spec, gain_spec, col_spec, col_spec, row_spec), out_specs=x_spec, check_vma=False)
```

```python
import functools

import jax
import jax.numpy as jnp
from jax import lax
from jax.experimental import pallas as pl
from jax.experimental.pallas import tpu as pltpu
from jax.sharding import PartitionSpec as P

MESH = pl.DeviceIdType.MESH
BF16 = jnp.bfloat16
F32 = jnp.float32
ANY = pl.BlockSpec(memory_space=pl.ANY)
VMEM_MAX = 67043328


def rope_tables(prefix, tokens, head_dim):
    positions = (prefix + jnp.arange(tokens)).astype(F32)
    inv_freq = 10000.0 ** (-2.0 * jnp.arange(head_dim // 2).astype(F32) / head_dim)
    angles = positions[:, None] * inv_freq[None, :]
    cos_half, sin_half = jnp.cos(angles), jnp.sin(angles)
    return jnp.concatenate([cos_half, cos_half], axis=-1), jnp.concatenate([-sin_half, sin_half], axis=-1)


NT = (((1,), (1,)), ((), ()))


def remote(src, dst, send_sem, recv_sem, **target):
    return pltpu.make_async_remote_copy(
        src_ref=src, dst_ref=dst, send_sem=send_sem, recv_sem=recv_sem, device_id=target, device_id_type=MESH
    )


def signal_all(targets):
    barrier = pltpu.get_barrier_semaphore()
    for target in targets:
        pl.semaphore_signal(barrier, inc=1, device_id=target, device_id_type=MESH)
    pl.semaphore_wait(barrier, len(targets))


PAIR = 256


def front_kernel(ring, owners, kv_ref, x_ref, wq_ref, wk_ref, wv_ref, wo_ref, gain_ref, cos_ref, sin_ref, mid_ref,
                 x_buf, normed, w_buf, proj, kv_buf, gathered, wo_buf, own_wo, total, mid_buf,
                 local_sem, w_sem, kv_send, kv_recv, a_send, a_recv, wo_send, wo_recv):
    me, here = lax.axis_index("heads"), lax.axis_index("pool")
    right, left = lax.rem(me + 1, ring), lax.rem(me + ring - 1, ring)
    tokens, width = x_ref.shape
    heads = kv_buf.shape[1]
    head_dim = kv_buf.shape[-1]
    prefix = owners * kv_buf.shape[2] * kv_buf.shape[4]
    block = width // ring
    half = tokens // 2
    scale = head_dim ** -0.5
    pairs = heads * head_dim // PAIR
    per_pair = PAIR // head_dim
    w_refs = (wq_ref, wk_ref, wv_ref)

    def load_pair(hp):
        cols = pl.ds(pl.multiple_of(hp * PAIR, PAIR), PAIR)
        slot = lax.rem(hp, 2)
        return [pltpu.make_async_copy(w_refs[m].at[:, cols], w_buf.at[slot, m], w_sem.at[slot, m]) for m in range(3)]

    x_copy = pltpu.make_async_copy(x_ref, x_buf, local_sem.at[0])
    x_copy.start()
    kv_own = pltpu.make_async_copy(kv_ref.at[here], kv_buf.at[here], local_sem.at[1])
    kv_own.start()
    for copy in load_pair(0):
        copy.start()
    wo_own = pltpu.make_async_copy(wo_ref.at[:, pl.ds(pl.multiple_of(me * block, block), block)], own_wo, local_sem.at[2])
    wo_own.start()

    signal_all([{"pool": lax.rem(here + t, owners)} for t in range(1, owners)] + [{"heads": lax.rem(me + u, ring)} for u in range(1, ring)])

    piece_rows = wo_ref.shape[0] // owners

    def wo_bring(u):
        dest = lax.rem(me + u, ring)
        src = wo_ref.at[pl.ds(pl.multiple_of(here * piece_rows, piece_rows), piece_rows), pl.ds(pl.multiple_of(dest * block, block), block)]
        return remote(src, wo_buf.at[u - 1, here], wo_send.at[u - 1], wo_recv.at[u - 1], heads=dest)

    chip_right, chip_left = lax.rem(here + 2, owners), lax.rem(here + owners - 2, owners)
    partner = here + 1 - 2 * lax.rem(here, 2)
    across = lax.rem(here + owners // 2, owners)
    half_rows = piece_rows // 2

    def wo_spread(i):
        piece = wo_buf.at[:, here]
        return remote(piece, piece, wo_send.at[3 + i], wo_recv.at[3 + i], pool=(chip_right, chip_left, partner)[i])

    def wo_onward(i):
        piece = wo_buf.at[:, (chip_left, chip_right)[i], pl.ds(i * half_rows, half_rows)]
        return remote(piece, piece, wo_send.at[6 + i], wo_recv.at[6 + i], pool=(chip_right, chip_left)[i])

    def wo_beside(i):
        piece = wo_buf.at[:, (chip_left, chip_right)[i]]
        return remote(piece, piece, wo_send.at[8 + i], wo_recv.at[8 + i], pool=partner)

    def wo_beside_far(i):
        piece = wo_buf.at[:, across, pl.ds(i * half_rows, half_rows)]
        return remote(piece, piece, wo_send.at[10 + i], wo_recv.at[10 + i], pool=partner)

    for u in range(1, ring):
        wo_bring(u).start()

    def page_copy(g, t):
        dest = lax.rem(here + t, owners)
        return remote(kv_ref.at[dest, g], kv_buf.at[here, g], kv_send.at[t - 1, g], kv_recv.at[t - 1, g], pool=dest)

    order = sorted(range(1, owners), key=lambda t: -min(t, owners - t))

    def send_pages(g, carry):
        for t in order:
            page_copy(g, t).start()
        return carry

    lax.fori_loop(0, heads, send_pages, 0)

    x_copy.wait()
    step = 64

    def normalise(i, carry):
        rows = pl.ds(pl.multiple_of(i * step, step), step)
        val = x_buf[rows].astype(F32)
        inv_rms = lax.rsqrt(jnp.mean(val * val, axis=-1, keepdims=True) + 1e-5)
        normed[rows] = (val * inv_rms * gain_ref[...].astype(F32)).astype(BF16)
        return carry

    lax.fori_loop(0, tokens // step, normalise, 0)
    kv_own.wait()

    def lanes(g):
        return pl.ds(pl.multiple_of(g * head_dim, head_dim), head_dim)

    def a_direct(g, way):
        piece = gathered.at[me, :, lanes(g)]
        return remote(piece, piece, a_send.at[g, 0, way], a_recv.at[g, 0, way], heads=(right, left)[way])

    def a_passed(g, way):
        piece = gathered.at[(left, right)[way], pl.ds(way * half, half), lanes(g)]
        return remote(piece, piece, a_send.at[g, 1, way], a_recv.at[g, 1, way], heads=(right, left)[way])

    def a_forward(g):
        for way in range(2):
            a_direct(g, way).wait_recv()
            a_passed(g, way).start()

    def rope(val):
        return (val * cos_ref[...] + pltpu.roll(val, head_dim // 2, 1) * sin_ref[...]).astype(BF16)

    def attend(hp, sub):
        g = hp * per_pair + sub
        cols = slice(sub * head_dim, (sub + 1) * head_dim)
        for t in range(1, owners):
            page_copy(g, t).wait_recv()
        keys_pre = kv_buf[:, g, :, 0].reshape(prefix, head_dim)
        vals_pre = kv_buf[:, g, :, 1].reshape(prefix, head_dim)
        for part in range(2):
            rows = slice(part * half, (part + 1) * half)
            seen = (part + 1) * half
            q_part = proj[0, rows, cols]
            s_pre = lax.dot_general(q_part, keys_pre, NT, preferred_element_type=F32) * scale
            s_new = lax.dot_general(q_part, proj[1, :seen, cols], NT, preferred_element_type=F32) * scale
            t_id = lax.broadcasted_iota(jnp.int32, s_new.shape, 0) + part * half
            u_id = lax.broadcasted_iota(jnp.int32, s_new.shape, 1)
            s_new = jnp.where(t_id >= u_id, s_new, -jnp.inf)
            row_max = jnp.maximum(jnp.max(s_pre, axis=-1, keepdims=True), jnp.max(s_new, axis=-1, keepdims=True))
            e_pre = jnp.exp(s_pre - row_max)
            e_new = jnp.exp(s_new - row_max)
            inv_den = 1.0 / (jnp.sum(e_pre, axis=-1, keepdims=True) + jnp.sum(e_new, axis=-1, keepdims=True))
            out = jnp.dot((e_pre * inv_den).astype(BF16), vals_pre, preferred_element_type=F32)
            out = out + jnp.dot((e_new * inv_den).astype(BF16), proj[2, :seen, cols], preferred_element_type=F32)
            gathered[me, rows, lanes(g)] = out.astype(BF16)
        for way in range(2):
            a_direct(g, way).start()

    def one_pair(hp, carry):
        for copy in load_pair(hp):
            copy.wait()

        @pl.when(hp + 1 < pairs)
        def _():
            for copy in load_pair(hp + 1):
                copy.start()

        slot = lax.rem(hp, 2)
        for m in range(3):
            val = jnp.dot(normed[...], w_buf[slot, m], preferred_element_type=F32)
            for sub in range(per_pair):
                cols = slice(sub * head_dim, (sub + 1) * head_dim)
                proj[m, :, cols] = rope(val[:, cols]) if m < 2 else val[:, cols].astype(BF16)
        for sub in range(per_pair):
            attend(hp, sub)
            g = hp * per_pair + sub

            @pl.when(g > 0)
            def _():
                a_forward(g - 1)

        @pl.when(hp == pairs // 2)
        def _():
            for u in range(1, ring):
                wo_bring(u).wait_recv()
            for i in range(3):
                wo_spread(i).start()

        return carry

    lax.fori_loop(0, pairs, one_pair, 0)
    a_forward(heads - 1)
    wo_own.wait()
    total[...] = jnp.dot(gathered[me], own_wo[...], preferred_element_type=F32)

    for i in range(2):
        wo_spread(i).wait_recv()
        wo_onward(i).start()
        wo_beside(i).start()

    def a_settle(g, carry):
        for way in range(2):
            a_direct(g, way).wait_send()
            a_passed(g, way).wait()
        return carry

    lax.fori_loop(0, heads, a_settle, 0)
    for i in range(2):
        wo_onward(i).wait_recv()
        wo_beside_far(i).start()
    wo_spread(2).wait_recv()
    for i in range(2):
        wo_beside(i).wait_recv()
    for i in range(2):
        wo_beside_far(i).wait_recv()

    for n in range(2):
        cols = slice(n * block // 2, (n + 1) * block // 2)
        res = total[:, cols]
        for u in range(1, ring):
            weight = wo_buf[u - 1, :, :, cols].reshape(owners * piece_rows, block // 2)
            res = res + jnp.dot(gathered[lax.rem(me + ring - u, ring)], weight, preferred_element_type=F32)
        x_cols = pl.ds(pl.multiple_of(me * block + n * (block // 2), block // 2), block // 2)
        mid_buf[:, cols] = (x_buf[:, x_cols].astype(F32) + res).astype(BF16)
    mid_copy = pltpu.make_async_copy(mid_buf, mid_ref, local_sem.at[0])
    mid_copy.start()

    def page_settle(g, carry):
        for t in range(1, owners):
            page_copy(g, t).wait_send()
        return carry

    lax.fori_loop(0, heads, page_settle, 0)
    for u in range(1, ring):
        wo_bring(u).wait_send()
    for i in range(3):
        wo_spread(i).wait_send()
    for i in range(2):
        wo_onward(i).wait_send()
        wo_beside(i).wait_send()
        wo_beside_far(i).wait_send()
    mid_copy.wait()


def front(call_id, ring, owners, kv, x, w_q, w_k, w_v, w_o, gain, cos_tab, sin_tab):
    tokens, width = x.shape
    heads, head_dim = kv.shape[1], kv.shape[-1]
    block = width // ring
    local = heads * head_dim
    dma = pltpu.SemaphoreType.DMA
    in_vmem = pl.BlockSpec(memory_space=pltpu.VMEM)
    return pl.pallas_call(
        functools.partial(front_kernel, ring, owners),
        out_shape=jax.ShapeDtypeStruct((tokens, block), BF16),
        in_specs=[ANY] * 6 + [in_vmem] * 3,
        out_specs=ANY,
        scratch_shapes=[
            pltpu.VMEM((tokens, width), BF16),
            pltpu.VMEM((tokens, width), BF16),
            pltpu.VMEM((2, 3, width, PAIR), BF16),
            pltpu.VMEM((3, tokens, PAIR), BF16),
            pltpu.VMEM(kv.shape, BF16),
            pltpu.VMEM((ring, tokens, local), BF16),
            pltpu.VMEM((ring - 1, owners, local // owners, block), BF16),
            pltpu.VMEM((local, block), BF16),
            pltpu.VMEM((tokens, block), F32),
            pltpu.VMEM((tokens, block), BF16),
            dma((3,)), dma((2, 3)),
            dma((owners - 1, heads)), dma((owners - 1, heads)),
            dma((heads, 2, 2)), dma((heads, 2, 2)),
            dma((12,)), dma((12,)),
        ],
        compiler_params=pltpu.CompilerParams(collective_id=call_id, has_side_effects=True, vmem_limit_bytes=VMEM_MAX),
        cost_estimate=pl.CostEstimate(flops=8 * tokens * width * local, bytes_accessed=48 * 2**20, transcendentals=heads * tokens * 3 * tokens),
        name="front",
    )(kv, x, w_q, w_k, w_v, w_o, gain, cos_tab, sin_tab)


CHUNKS = 2
GROUPS = 4
N_BLOCK = 256


def mlp_kernel(ring, x_ref, gain_ref, wg_ref, wu_ref, wd_ref, out_ref,
               mid, normed, gate_w, up_w, act, down_w, part_sum, running, result,
               local_sem, w_sem, d_sem, mid_send, mid_recv, rs_send, rs_recv, ag_send, ag_recv, out_sem):
    me = lax.axis_index("heads")
    right, left = lax.rem(me + 1, ring), lax.rem(me + ring - 1, ring)
    ways = (right, left)
    tokens, block = x_ref.shape
    width = block * ring
    hid = wg_ref.shape[0]
    rows_c = tokens // CHUNKS
    rows_g = tokens // GROUPS
    per_chunk = GROUPS // CHUNKS
    n_half = block // 2
    n_full, n_rest = hid // N_BLOCK, hid % N_BLOCK
    n_steps = n_full + 1

    x_copies = []
    for c in range(CHUNKS):
        rows = pl.ds(c * rows_c, rows_c)
        x_copies.append(pltpu.make_async_copy(x_ref.at[rows], mid.at[me, rows], local_sem.at[c]))
        x_copies[c].start()

    def load_full(c, i):
        rows = pl.ds(pl.multiple_of(i * N_BLOCK, N_BLOCK), N_BLOCK)
        slot = lax.rem(c * n_steps + i, 3)
        return (pltpu.make_async_copy(wg_ref.at[rows], gate_w.at[slot], w_sem.at[0, slot]),
                pltpu.make_async_copy(wu_ref.at[rows], up_w.at[slot], w_sem.at[1, slot]))

    def load_rest(c):
        rows, dst = pl.ds(n_full * N_BLOCK, n_rest), pl.ds(0, n_rest)
        slot = (c * n_steps + n_full) % 3
        return (pltpu.make_async_copy(wg_ref.at[rows], gate_w.at[slot, dst], w_sem.at[0, slot]),
                pltpu.make_async_copy(wu_ref.at[rows], up_w.at[slot, dst], w_sem.at[1, slot]))

    def run(copies):
        for copy in copies:
            copy.start()

    def load_down(jj):
        s, way = lax.rem(jj // 2, ring), lax.rem(jj, 2)
        blk = jnp.where(way == 0, lax.rem(me + 2 * ring - 1 - s, ring), lax.rem(me + 1 + s, ring))
        col = pl.multiple_of(blk * block + way * n_half, n_half)
        slot = lax.rem(jj, 3)
        return pltpu.make_async_copy(wd_ref.at[:, pl.ds(col, n_half)], down_w.at[slot], d_sem.at[slot])

    run(load_full(0, 0))
    run(load_full(0, 1))
    for jj in range(2):
        load_down(jj).start()

    signal_all([{"heads": right}, {"heads": left}])

    def mid_direct(c, way):
        piece = mid.at[me, pl.ds(c * rows_c, rows_c)]
        return remote(piece, piece, mid_send.at[c, 0, way], mid_recv.at[c, 0, way], heads=ways[way])

    def mid_passed(c, way):
        piece = mid.at[(left, right)[way], pl.ds(c * rows_c + way * (rows_c // 2), rows_c // 2)]
        return remote(piece, piece, mid_send.at[c, 1, way], mid_recv.at[c, 1, way], heads=ways[way])

    def mid_start(c):
        x_copies[c].wait()
        for way in range(2):
            mid_direct(c, way).start()

    def mid_forward(c):
        for way in range(2):
            mid_direct(c, way).wait_recv()
            mid_passed(c, way).start()

    def mid_settle(c):
        for way in range(2):
            mid_passed(c, way).wait_recv()

    def rs_send_copy(r, s, way):
        rows = pl.ds((r % per_chunk) * rows_g, rows_g)
        src = part_sum.at[r // per_chunk, 0, way, rows] if s == 0 else running.at[r, s - 1, way]
        return remote(src, running.at[r, s, way], rs_send.at[r, s, way], rs_recv.at[r, s, way], heads=ways[way])

    def rs_step(r, s):
        rows = slice((r % per_chunk) * rows_g, (r % per_chunk + 1) * rows_g)
        for way in range(2):
            rs_send_copy(r, s - 1, way).wait_recv()
            running[r, s - 1, way] = running[r, s - 1, way] + part_sum[r // per_chunk, s, way, rows]
            rs_send_copy(r, s, way).start()

    def ag_direct(r, way):
        piece = result.at[me, pl.ds(r * rows_g, rows_g)]
        return remote(piece, piece, ag_send.at[r, 0, way], ag_recv.at[r, 0, way], heads=ways[way])

    def ag_passed(r, way):
        piece = result.at[(left, right)[way], pl.ds(r * rows_g + way * (rows_g // 2), rows_g // 2)]
        return remote(piece, piece, ag_send.at[r, 1, way], ag_recv.at[r, 1, way], heads=ways[way])

    def rs_final(r):
        rows = slice((r % per_chunk) * rows_g, (r % per_chunk + 1) * rows_g)
        dst = slice(r * rows_g, (r + 1) * rows_g)
        for way in range(2):
            rs_send_copy(r, ring - 2, way).wait_recv()
            cols = slice(way * n_half, (way + 1) * n_half)
            total = running[r, ring - 2, way] + part_sum[r // per_chunk, ring - 1, way, rows]
            result[me, dst, cols] = (mid[me, dst, cols].astype(F32) + total).astype(BF16)
        for way in range(2):
            ag_direct(r, way).start()

    def ag_forward(r):
        for way in range(2):
            ag_direct(r, way).wait_recv()
            ag_passed(r, way).start()

    def put_out(r, src):
        rows = pl.ds(r * rows_g, rows_g)
        return pltpu.make_async_copy(result.at[src, rows], out_ref.at[rows, pl.ds(src * block, block)], out_sem.at[r, src])

    def ag_settle(r):
        for way in range(2):
            ag_passed(r, way).wait_recv()
        for src in range(ring):
            put_out(r, src).start()

    def normalise(c):
        step = 64

        def body(i, carry):
            base = pl.multiple_of(i * step, step)
            rows, out_rows = pl.ds(c * rows_c + base, step), pl.ds(base, step)
            squares = jnp.zeros((step, 1), F32)
            for b in range(ring):
                val = mid[b, rows].astype(F32)
                squares = squares + jnp.sum(val * val, axis=-1, keepdims=True)
            inv_rms = lax.rsqrt(squares * (1.0 / width) + 1e-5)
            for b in range(ring):
                cols = slice(b * block, (b + 1) * block)
                normed[out_rows, cols] = (mid[b, rows].astype(F32) * inv_rms * gain_ref[:, cols].astype(F32)).astype(BF16)
            return carry

        lax.fori_loop(0, rows_c // step, body, 0)

    def hidden_block(gate_rows, up_rows):
        gate = lax.dot_general(normed[...], gate_rows, NT, preferred_element_type=F32)
        up = lax.dot_general(normed[...], up_rows, NT, preferred_element_type=F32)
        return (gate * jax.nn.sigmoid(gate) * up).astype(BF16)

    def gate_up(c, tasks):
        def body(i, carry):
            slot = lax.rem(c * n_steps + i, 3)
            for copy in load_full(c, i):
                copy.wait()
            pl.when(i + 2 < n_full)(lambda: run(load_full(c, i + 2)))
            pl.when(i + 2 == n_full)(lambda: run(load_rest(c)))
            if c + 1 < CHUNKS:
                pl.when(i + 2 == n_full + 1)(lambda: run(load_full(c + 1, 0)))
            act[:, pl.ds(pl.multiple_of(i * N_BLOCK, N_BLOCK), N_BLOCK)] = hidden_block(gate_w[slot], up_w[slot])
            for at, task in tasks:
                pl.when(i == at)(task)
            return carry

        lax.fori_loop(0, n_full, body, 0)
        for copy in load_rest(c):
            copy.wait()
        if c + 1 < CHUNKS:
            run(load_full(c + 1, 1))
        slot = (c * n_steps + n_full) % 3
        act[:, n_full * N_BLOCK:] = hidden_block(gate_w[slot, :n_rest], up_w[slot, :n_rest])

    def down(c, tasks):
        def body(s, carry):
            for way in range(2):
                jj = c * 2 * ring + 2 * s + way
                load_down(jj).wait()
                pl.when(jj + 2 < CHUNKS * 2 * ring)(lambda: load_down(jj + 2).start())
                part_sum[c, s, way] = jnp.dot(act[...], down_w[lax.rem(jj, 3)], preferred_element_type=F32)

            @pl.when(s == 0)
            def _():
                for sub in range(per_chunk):
                    for way in range(2):
                        rs_send_copy(c * per_chunk + sub, 0, way).start()

            for at, task in tasks:
                pl.when(s == at)(task)
            return carry

        lax.fori_loop(0, ring, body, 0)

    do = functools.partial
    mid_start(0)
    mid_forward(0)
    mid_start(1)
    mid_settle(0)
    normalise(0)
    gate_up(0, [(7, do(mid_forward, 1))])
    down(0, [])
    mid_settle(1)
    normalise(1)
    gate_up(1, [(2, do(rs_step, 0, 1)), (5, do(rs_step, 1, 1)), (8, do(rs_step, 0, 2))])
    down(1, [(0, do(rs_step, 1, 2)), (2, do(rs_final, 0)), (3, do(rs_final, 1))])
    rs_step(2, 1)
    rs_step(3, 1)
    ag_forward(0)
    ag_forward(1)
    rs_step(2, 2)
    rs_step(3, 2)
    ag_settle(0)
    ag_settle(1)
    rs_final(2)
    rs_final(3)
    ag_forward(2)
    ag_forward(3)
    ag_settle(2)
    ag_settle(3)
    for c in range(CHUNKS):
        for way in range(2):
            mid_direct(c, way).wait_send()
            mid_passed(c, way).wait_send()
    for r in range(GROUPS):
        for way in range(2):
            for s in range(ring - 1):
                rs_send_copy(r, s, way).wait_send()
            ag_direct(r, way).wait_send()
            ag_passed(r, way).wait_send()
        for src in range(ring):
            put_out(r, src).wait()


def mlp(call_id, ring, x_mid, gain, w_gate, w_up, w_down):
    tokens, block = x_mid.shape
    hid, width = w_gate.shape
    rows_c, rows_g = tokens // CHUNKS, tokens // GROUPS
    dma = pltpu.SemaphoreType.DMA
    return pl.pallas_call(
        functools.partial(mlp_kernel, ring),
        out_shape=jax.ShapeDtypeStruct((tokens, width), BF16),
        in_specs=[ANY, pl.BlockSpec(memory_space=pltpu.VMEM), ANY, ANY, ANY],
        out_specs=ANY,
        scratch_shapes=[
            pltpu.VMEM((ring, tokens, block), BF16),
            pltpu.VMEM((rows_c, width), BF16),
            pltpu.VMEM((3, N_BLOCK, width), BF16),
            pltpu.VMEM((3, N_BLOCK, width), BF16),
            pltpu.VMEM((rows_c, hid), BF16),
            pltpu.VMEM((3, hid, block // 2), BF16),
            pltpu.VMEM((CHUNKS, ring, 2, rows_c, block // 2), F32),
            pltpu.VMEM((GROUPS, ring - 1, 2, rows_g, block // 2), F32),
            pltpu.VMEM((ring, tokens, block), BF16),
            dma((CHUNKS,)), dma((2, 3)), dma((3,)),
            dma((CHUNKS, 2, 2)), dma((CHUNKS, 2, 2)),
            dma((GROUPS, ring - 1, 2)), dma((GROUPS, ring - 1, 2)),
            dma((GROUPS, 2, 2)), dma((GROUPS, 2, 2)),
            dma((GROUPS, ring)),
        ],
        compiler_params=pltpu.CompilerParams(collective_id=call_id, has_side_effects=True, vmem_limit_bytes=VMEM_MAX),
        cost_estimate=pl.CostEstimate(flops=6 * tokens * width * hid, bytes_accessed=140 * 2**20, transcendentals=tokens * hid),
        name="mlp",
    )(x_mid, gain, w_gate, w_up, w_down)


def solution(mesh):
    owners = mesh.shape["pool"]
    ring = mesh.shape["heads"]
    assert ring == 4 and owners == 8

    def local_fn(kv_pool, page_idx, x_tokens, gain_attn, w_q, w_k, w_v, w_o, gain_mlp, w_gate, w_up, w_down):
        layers, _, _, page_len, kv_loc, head_dim = kv_pool.shape
        tokens = x_tokens.shape[1]
        req_pages = page_idx.shape[2]
        wanted = page_idx.reshape(owners * req_pages)
        cos_tab, sin_tab = rope_tables(owners * req_pages * page_len, tokens, head_dim)
        hidden = x_tokens[0]
        for layer in range(layers):
            picked = kv_pool.at[layer, wanted].get(mode="promise_in_bounds")
            picked = picked.reshape(owners, req_pages, 2, page_len, kv_loc, head_dim).transpose(0, 4, 1, 2, 3, 5)
            x_mid = front(2 * layer, ring, owners, picked, hidden, w_q[layer], w_k[layer], w_v[layer], w_o[layer], gain_attn[layer][None], cos_tab, sin_tab)
            hidden = mlp(2 * layer + 1, ring, x_mid, gain_mlp[layer][None], w_gate[layer].T, w_up[layer].T, w_down[layer])
        return hidden[None]

    pool_spec = P(None, ("rep", "pool"), None, None, "heads", None)
    index_spec = P("rep", "pool", None)
    x_spec = P(("rep", "pool"), None, None)
    gain_spec = P(None, None)
    col_spec = P(None, None, "heads")
    row_spec = P(None, "heads", None)
    return jax.shard_map(local_fn, mesh=mesh, in_specs=(pool_spec, index_spec, x_spec, gain_spec, col_spec, col_spec, col_spec, row_spec, gain_spec, col_spec, col_spec, row_spec), out_specs=x_spec, check_vma=False)
```

```python
import functools

import jax
import jax.numpy as jnp
import numpy as np
from jax import lax
from jax.experimental import pallas as pl
from jax.experimental.pallas import tpu as pltpu
from jax.sharding import PartitionSpec as P

MESH = pl.DeviceIdType.MESH
BF16 = jnp.bfloat16
F32 = jnp.float32
ANY = pl.BlockSpec(memory_space=pl.ANY)
VMEM_MAX = 67043328


def rope_tables(prefix, tokens, head_dim):
    positions = (prefix + np.arange(tokens)).astype(np.float32)
    inv_freq = np.float32(10000.0) ** (-2.0 * np.arange(head_dim // 2).astype(np.float32) / head_dim).astype(np.float32)
    angles = positions[:, None] * inv_freq[None, :]
    cos_half, sin_half = np.cos(angles), np.sin(angles)
    return np.concatenate([cos_half, cos_half], axis=-1), np.concatenate([-sin_half, sin_half], axis=-1)


def pick_kernel(idx_ref, page_ref, out_ref):
    for side in range(2):
        out_ref[0, :, 0, side] = jnp.swapaxes(page_ref[0, side], 0, 1)


def pick_pages(pool, wanted, owners):
    _, _, page_len, heads, head_dim = pool.shape
    each = wanted.shape[0] // owners
    return pl.pallas_call(
        pick_kernel,
        grid_spec=pltpu.PrefetchScalarGridSpec(
            num_scalar_prefetch=1,
            grid=(wanted.shape[0],),
            in_specs=[pl.BlockSpec((1, 2, page_len, heads, head_dim), lambda i, idx: (idx[i], 0, 0, 0, 0))],
            out_specs=pl.BlockSpec((1, heads, 1, 2, page_len, head_dim), lambda i, idx: (i // each, 0, i % each, 0, 0, 0)),
        ),
        out_shape=jax.ShapeDtypeStruct((owners, heads, each, 2, page_len, head_dim), pool.dtype),
        name="pick_pages",
    )(wanted, pool)


NT = (((1,), (1,)), ((), ()))


def remote(src, dst, send_sem, recv_sem, **target):
    return pltpu.make_async_remote_copy(
        src_ref=src, dst_ref=dst, send_sem=send_sem, recv_sem=recv_sem, device_id=target, device_id_type=MESH
    )


def signal_all(targets):
    barrier = pltpu.get_barrier_semaphore()
    for target in targets:
        pl.semaphore_signal(barrier, inc=1, device_id=target, device_id_type=MESH)
    pl.semaphore_wait(barrier, len(targets))


PAIR = 256
SPREAD = 64


def front_kernel(ring, owners, kv_ref, x_ref, wq_ref, wk_ref, wv_ref, wo_ref, gain_ref, cos_ref, sin_ref, mid_ref,
                 x_buf, normed, w_buf, proj, kv_buf, gathered, wo_buf, own_wo, total, mid_buf,
                 local_sem, w_sem, kv_send, kv_recv, a_send, a_recv, wo_send, wo_recv, rest_send, rest_recv):
    me, here = lax.axis_index("heads"), lax.axis_index("pool")
    right, left = lax.rem(me + 1, ring), lax.rem(me + ring - 1, ring)
    tokens, width = x_ref.shape
    heads = kv_buf.shape[1]
    head_dim = kv_buf.shape[-1]
    prefix = owners * kv_buf.shape[2] * kv_buf.shape[4]
    block = width // ring
    half = tokens // 2
    scale = head_dim ** -0.5
    pairs = heads * head_dim // PAIR
    per_pair = PAIR // head_dim
    w_refs = (wq_ref, wk_ref, wv_ref)

    def load_pair(hp):
        cols = pl.ds(pl.multiple_of(hp * PAIR, PAIR), PAIR)
        slot = lax.rem(hp, 2)
        return [pltpu.make_async_copy(w_refs[m].at[:, cols], w_buf.at[slot, m], w_sem.at[slot, m]) for m in range(3)]

    x_copy = pltpu.make_async_copy(x_ref, x_buf, local_sem.at[0])
    x_copy.start()
    kv_own = pltpu.make_async_copy(kv_ref.at[here], kv_buf.at[here], local_sem.at[1])
    kv_own.start()
    for copy in load_pair(0):
        copy.start()
    wo_own = pltpu.make_async_copy(wo_ref.at[:, pl.ds(pl.multiple_of(me * block, block), block)], own_wo, local_sem.at[2])
    wo_own.start()

    signal_all([{"pool": lax.rem(here + t, owners)} for t in range(1, owners)] + [{"heads": lax.rem(me + u, ring)} for u in range(1, ring)])

    piece_rows = wo_ref.shape[0] // owners
    spread_rows = pl.ds(0, SPREAD)
    core = lax.rem(here, 2)
    partner = here + 1 - 2 * core
    chip_right, chip_left = lax.rem(here + 2, owners), lax.rem(here + owners - 2, owners)
    across = lax.rem(here + owners // 2, owners)

    def wo_columns(u, row, rows):
        dest = lax.rem(me + u, ring)
        return dest, wo_ref.at[pl.ds(pl.multiple_of(row, 16), rows), pl.ds(pl.multiple_of(dest * block, block), block)]

    def wo_bring(u):
        dest, src = wo_columns(u, here * piece_rows, SPREAD)
        return remote(src, wo_buf.at[u - 1, here, spread_rows], wo_send.at[u - 1], wo_recv.at[u - 1], heads=dest)

    def wo_spread(i):
        piece = wo_buf.at[:, here, spread_rows]
        return remote(piece, piece, wo_send.at[3 + i], wo_recv.at[3 + i], pool=(chip_right, chip_left, partner)[i])

    def wo_onward(i):
        piece = wo_buf.at[:, (chip_left, chip_right)[i], pl.ds(i * (SPREAD // 2), SPREAD // 2)]
        return remote(piece, piece, wo_send.at[6 + i], wo_recv.at[6 + i], pool=(chip_right, chip_left)[i])

    def wo_beside(i):
        piece = wo_buf.at[:, (chip_left, chip_right)[i], spread_rows]
        return remote(piece, piece, wo_send.at[8 + i], wo_recv.at[8 + i], pool=partner)

    def wo_beside_far(i):
        piece = wo_buf.at[:, across, pl.ds(i * (SPREAD // 2), SPREAD // 2)]
        return remote(piece, piece, wo_send.at[10 + i], wo_recv.at[10 + i], pool=partner)

    rest = piece_rows - SPREAD
    rest_rows = pl.ds(SPREAD, rest)
    chips = owners // 2

    def wo_rest(u, i):
        piece = 2 * i + core
        dest, src = wo_columns(u, piece * piece_rows + SPREAD, rest)
        return remote(src, wo_buf.at[u - 1, piece, rest_rows], rest_send.at[u - 1, i], rest_recv.at[u - 1, i], heads=dest)

    def wo_hand(i):
        piece = wo_buf.at[:, 2 * i + core, rest_rows]
        return remote(piece, piece, rest_send.at[ring - 1, i], rest_recv.at[ring - 1, i], pool=partner)

    for u in range(1, ring):
        wo_bring(u).start()
    def rest_start(i):
        for u in (2, 1, 3):
            wo_rest(u, i).start()

    early = chips // 2
    for i in range(early):
        rest_start(i)

    def page_copy(g, t):
        dest = lax.rem(here + t, owners)
        return remote(kv_ref.at[dest, g], kv_buf.at[here, g], kv_send.at[t - 1, g], kv_recv.at[t - 1, g], pool=dest)

    order = sorted(range(1, owners), key=lambda t: -min(t, owners - t))

    def send_pages(g, carry):
        for t in order:
            page_copy(g, t).start()
        return carry

    lax.fori_loop(0, heads, send_pages, 0)

    x_copy.wait()
    step = 64

    def normalise(i, carry):
        rows = pl.ds(pl.multiple_of(i * step, step), step)
        val = x_buf[rows].astype(F32)
        inv_rms = lax.rsqrt(jnp.mean(val * val, axis=-1, keepdims=True) + 1e-5)
        normed[rows] = (val * inv_rms * gain_ref[...].astype(F32)).astype(BF16)
        return carry

    lax.fori_loop(0, tokens // step, normalise, 0)
    kv_own.wait()

    def all_heads(src):
        return jnp.concatenate([gathered[src, g] for g in range(heads)], axis=-1)

    def a_direct(g, way):
        piece = gathered.at[me, g]
        return remote(piece, piece, a_send.at[g, 0, way], a_recv.at[g, 0, way], heads=(right, left)[way])

    def a_passed(g, way):
        piece = gathered.at[(left, right)[way], g, pl.ds(way * half, half)]
        return remote(piece, piece, a_send.at[g, 1, way], a_recv.at[g, 1, way], heads=(right, left)[way])

    def a_forward(g):
        for way in range(2):
            a_direct(g, way).wait_recv()
            a_passed(g, way).start()

    def rope(val):
        return (val * cos_ref[...] + pltpu.roll(val, head_dim // 2, 1) * sin_ref[...]).astype(BF16)

    def attend(hp, sub):
        g = hp * per_pair + sub
        cols = slice(sub * head_dim, (sub + 1) * head_dim)
        for t in range(1, owners):
            page_copy(g, t).wait_recv()
        keys_pre = kv_buf[:, g, :, 0].reshape(prefix, head_dim)
        vals_pre = kv_buf[:, g, :, 1].reshape(prefix, head_dim)
        for part in range(2):
            rows = slice(part * half, (part + 1) * half)
            seen = (part + 1) * half
            q_part = proj[0, rows, cols]
            s_pre = lax.dot_general(q_part, keys_pre, NT, preferred_element_type=F32) * scale
            s_new = lax.dot_general(q_part, proj[1, :seen, cols], NT, preferred_element_type=F32) * scale
            t_id = lax.broadcasted_iota(jnp.int32, s_new.shape, 0) + part * half
            u_id = lax.broadcasted_iota(jnp.int32, s_new.shape, 1)
            s_new = jnp.where(t_id >= u_id, s_new, -jnp.inf)
            row_max = jnp.maximum(jnp.max(s_pre, axis=-1, keepdims=True), jnp.max(s_new, axis=-1, keepdims=True))
            e_pre = jnp.exp(s_pre - row_max)
            e_new = jnp.exp(s_new - row_max)
            inv_den = 1.0 / (jnp.sum(e_pre, axis=-1, keepdims=True) + jnp.sum(e_new, axis=-1, keepdims=True))
            out = jnp.dot((e_pre * inv_den).astype(BF16), vals_pre, preferred_element_type=F32)
            out = out + jnp.dot((e_new * inv_den).astype(BF16), proj[2, :seen, cols], preferred_element_type=F32)
            gathered[me, g, rows] = out.astype(BF16)
        for way in range(2):
            a_direct(g, way).start()

    def one_pair(hp, carry):
        for copy in load_pair(hp):
            copy.wait()

        @pl.when(hp + 1 < pairs)
        def _():
            for copy in load_pair(hp + 1):
                copy.start()

        slot = lax.rem(hp, 2)
        for m in range(3):
            val = jnp.dot(normed[...], w_buf[slot, m], preferred_element_type=F32)
            for sub in range(per_pair):
                cols = slice(sub * head_dim, (sub + 1) * head_dim)
                proj[m, :, cols] = rope(val[:, cols]) if m < 2 else val[:, cols].astype(BF16)
        for sub in range(per_pair):
            attend(hp, sub)
            g = hp * per_pair + sub

            @pl.when(g >= per_pair)
            def _():
                a_forward(g - per_pair)

        for i in range(early, chips):
            pl.when(hp == i - early)(functools.partial(rest_start, i))

        @pl.when(hp == 1)
        def _():
            for u in range(1, ring):
                wo_bring(u).wait_recv()
            for i in range(3):
                wo_spread(i).start()

        return carry

    lax.fori_loop(0, pairs, one_pair, 0)
    wo_own.wait()
    total[...] = jnp.dot(all_heads(me), own_wo[...], preferred_element_type=F32)
    for g in range(heads - per_pair, heads):
        a_forward(g)
    for i in range(chips):
        for u in range(1, ring):
            wo_rest(u, i).wait_recv()
        wo_hand(i).start()

    for i in range(2):
        wo_spread(i).wait_recv()
        wo_onward(i).start()
        wo_beside(i).start()

    def a_settle(g, carry):
        for way in range(2):
            a_direct(g, way).wait_send()
            a_passed(g, way).wait()
        return carry

    lax.fori_loop(0, heads, a_settle, 0)
    for i in range(2):
        wo_onward(i).wait_recv()
        wo_beside_far(i).start()
    wo_spread(2).wait_recv()
    for i in range(2):
        wo_beside(i).wait_recv()
    for i in range(2):
        wo_beside_far(i).wait_recv()
    for i in range(chips):
        wo_hand(i).wait_recv()

    for n in range(2):
        cols = slice(n * block // 2, (n + 1) * block // 2)
        res = total[:, cols]
        for u in range(1, ring):
            weight = wo_buf[u - 1, :, :, cols].reshape(owners * piece_rows, block // 2)
            res = res + jnp.dot(all_heads(lax.rem(me + ring - u, ring)), weight, preferred_element_type=F32)
        x_cols = pl.ds(pl.multiple_of(me * block + n * (block // 2), block // 2), block // 2)
        mid_buf[:, cols] = (x_buf[:, x_cols].astype(F32) + res).astype(BF16)
    mid_copy = pltpu.make_async_copy(mid_buf, mid_ref, local_sem.at[0])
    mid_copy.start()

    def page_settle(g, carry):
        for t in range(1, owners):
            page_copy(g, t).wait_send()
        return carry

    lax.fori_loop(0, heads, page_settle, 0)
    for u in range(1, ring):
        wo_bring(u).wait_send()
    for i in range(chips):
        for u in range(1, ring):
            wo_rest(u, i).wait_send()
        wo_hand(i).wait_send()
    for i in range(3):
        wo_spread(i).wait_send()
    for i in range(2):
        wo_onward(i).wait_send()
        wo_beside(i).wait_send()
        wo_beside_far(i).wait_send()
    mid_copy.wait()


def front(call_id, ring, owners, kv, x, w_q, w_k, w_v, w_o, gain, cos_tab, sin_tab):
    tokens, width = x.shape
    heads, head_dim = kv.shape[1], kv.shape[-1]
    block = width // ring
    local = heads * head_dim
    dma = pltpu.SemaphoreType.DMA
    in_vmem = pl.BlockSpec(memory_space=pltpu.VMEM)
    return pl.pallas_call(
        functools.partial(front_kernel, ring, owners),
        out_shape=jax.ShapeDtypeStruct((tokens, block), BF16),
        in_specs=[ANY] * 6 + [in_vmem] * 3,
        out_specs=ANY,
        scratch_shapes=[
            pltpu.VMEM((tokens, width), BF16),
            pltpu.VMEM((tokens, width), BF16),
            pltpu.VMEM((2, 3, width, PAIR), BF16),
            pltpu.VMEM((3, tokens, PAIR), BF16),
            pltpu.VMEM(kv.shape, BF16),
            pltpu.VMEM((ring, heads, tokens, head_dim), BF16),
            pltpu.VMEM((ring - 1, owners, local // owners, block), BF16),
            pltpu.VMEM((local, block), BF16),
            pltpu.VMEM((tokens, block), F32),
            pltpu.VMEM((tokens, block), BF16),
            dma((3,)), dma((2, 3)),
            dma((owners - 1, heads)), dma((owners - 1, heads)),
            dma((heads, 2, 2)), dma((heads, 2, 2)),
            dma((12,)), dma((12,)),
            dma((ring, owners // 2)), dma((ring, owners // 2)),
        ],
        compiler_params=pltpu.CompilerParams(collective_id=call_id, has_side_effects=True, vmem_limit_bytes=VMEM_MAX),
        cost_estimate=pl.CostEstimate(flops=8 * tokens * width * local, bytes_accessed=48 * 2**20, transcendentals=heads * tokens * 3 * tokens),
        name="front",
    )(kv, x, w_q, w_k, w_v, w_o, gain, cos_tab, sin_tab)


CHUNKS = 2
GROUPS = 4
N_BLOCK = 256


def mlp_kernel(ring, x_ref, gain_ref, wg_ref, wu_ref, wd_ref, out_ref,
               mid, normed, gate_w, up_w, act, down_w, part_sum, running, result,
               local_sem, w_sem, d_sem, mid_send, mid_recv, rs_send, rs_recv, ag_send, ag_recv, out_sem):
    me = lax.axis_index("heads")
    right, left = lax.rem(me + 1, ring), lax.rem(me + ring - 1, ring)
    ways = (right, left)
    tokens, block = x_ref.shape
    width = block * ring
    hid = wg_ref.shape[0]
    rows_c = tokens // CHUNKS
    rows_g = tokens // GROUPS
    per_chunk = GROUPS // CHUNKS
    n_half = block // 2
    n_full, n_rest = hid // N_BLOCK, hid % N_BLOCK
    n_steps = n_full + 1

    x_copies = []
    for c in range(CHUNKS):
        rows = pl.ds(c * rows_c, rows_c)
        x_copies.append(pltpu.make_async_copy(x_ref.at[rows], mid.at[me, rows], local_sem.at[c]))
        x_copies[c].start()

    def load_full(c, i):
        rows = pl.ds(pl.multiple_of(i * N_BLOCK, N_BLOCK), N_BLOCK)
        slot = lax.rem(c * n_steps + i, 3)
        return (pltpu.make_async_copy(wg_ref.at[rows], gate_w.at[slot], w_sem.at[0, slot]),
                pltpu.make_async_copy(wu_ref.at[rows], up_w.at[slot], w_sem.at[1, slot]))

    def load_rest(c):
        rows, dst = pl.ds(n_full * N_BLOCK, n_rest), pl.ds(0, n_rest)
        slot = (c * n_steps + n_full) % 3
        return (pltpu.make_async_copy(wg_ref.at[rows], gate_w.at[slot, dst], w_sem.at[0, slot]),
                pltpu.make_async_copy(wu_ref.at[rows], up_w.at[slot, dst], w_sem.at[1, slot]))

    def run(copies):
        for copy in copies:
            copy.start()

    def load_down(jj):
        s, way = lax.rem(jj // 2, ring), lax.rem(jj, 2)
        blk = jnp.where(way == 0, lax.rem(me + 2 * ring - 1 - s, ring), lax.rem(me + 1 + s, ring))
        col = pl.multiple_of(blk * block + way * n_half, n_half)
        slot = lax.rem(jj, 3)
        return pltpu.make_async_copy(wd_ref.at[:, pl.ds(col, n_half)], down_w.at[slot], d_sem.at[slot])

    run(load_full(0, 0))
    run(load_full(0, 1))
    for jj in range(2):
        load_down(jj).start()

    signal_all([{"heads": right}, {"heads": left}])

    def mid_direct(c, way):
        piece = mid.at[me, pl.ds(c * rows_c, rows_c)]
        return remote(piece, piece, mid_send.at[c, 0, way], mid_recv.at[c, 0, way], heads=ways[way])

    def mid_passed(c, way):
        piece = mid.at[(left, right)[way], pl.ds(c * rows_c + way * (rows_c // 2), rows_c // 2)]
        return remote(piece, piece, mid_send.at[c, 1, way], mid_recv.at[c, 1, way], heads=ways[way])

    def mid_start(c):
        x_copies[c].wait()
        for way in range(2):
            mid_direct(c, way).start()

    def mid_forward(c):
        for way in range(2):
            mid_direct(c, way).wait_recv()
            mid_passed(c, way).start()

    def mid_settle(c):
        for way in range(2):
            mid_passed(c, way).wait_recv()

    def rs_send_copy(r, s, way):
        rows = pl.ds((r % per_chunk) * rows_g, rows_g)
        src = part_sum.at[r // per_chunk, 0, way, rows] if s == 0 else running.at[r, s - 1, way]
        return remote(src, running.at[r, s, way], rs_send.at[r, s, way], rs_recv.at[r, s, way], heads=ways[way])

    def rs_step(r, s):
        rows = slice((r % per_chunk) * rows_g, (r % per_chunk + 1) * rows_g)
        for way in range(2):
            rs_send_copy(r, s - 1, way).wait_recv()
            running[r, s - 1, way] = running[r, s - 1, way] + part_sum[r // per_chunk, s, way, rows]
            rs_send_copy(r, s, way).start()

    def ag_direct(r, way):
        piece = result.at[me, pl.ds(r * rows_g, rows_g)]
        return remote(piece, piece, ag_send.at[r, 0, way], ag_recv.at[r, 0, way], heads=ways[way])

    def ag_passed(r, way):
        piece = result.at[(left, right)[way], pl.ds(r * rows_g + way * (rows_g // 2), rows_g // 2)]
        return remote(piece, piece, ag_send.at[r, 1, way], ag_recv.at[r, 1, way], heads=ways[way])

    def rs_final(r):
        rows = slice((r % per_chunk) * rows_g, (r % per_chunk + 1) * rows_g)
        dst = slice(r * rows_g, (r + 1) * rows_g)
        for way in range(2):
            rs_send_copy(r, ring - 2, way).wait_recv()
            cols = slice(way * n_half, (way + 1) * n_half)
            total = running[r, ring - 2, way] + part_sum[r // per_chunk, ring - 1, way, rows]
            result[me, dst, cols] = (mid[me, dst, cols].astype(F32) + total).astype(BF16)
        for way in range(2):
            ag_direct(r, way).start()

    def ag_forward(r):
        for way in range(2):
            ag_direct(r, way).wait_recv()
            ag_passed(r, way).start()

    def put_out(r, src):
        rows = pl.ds(r * rows_g, rows_g)
        return pltpu.make_async_copy(result.at[src, rows], out_ref.at[rows, pl.ds(src * block, block)], out_sem.at[r, src])

    def ag_settle(r):
        for way in range(2):
            ag_passed(r, way).wait_recv()
        for src in range(ring):
            put_out(r, src).start()

    def normalise(c):
        step = 64

        def body(i, carry):
            base = pl.multiple_of(i * step, step)
            rows, out_rows = pl.ds(c * rows_c + base, step), pl.ds(base, step)
            squares = jnp.zeros((step, 1), F32)
            for b in range(ring):
                val = mid[b, rows].astype(F32)
                squares = squares + jnp.sum(val * val, axis=-1, keepdims=True)
            inv_rms = lax.rsqrt(squares * (1.0 / width) + 1e-5)
            for b in range(ring):
                cols = slice(b * block, (b + 1) * block)
                normed[out_rows, cols] = (mid[b, rows].astype(F32) * inv_rms * gain_ref[:, cols].astype(F32)).astype(BF16)
            return carry

        lax.fori_loop(0, rows_c // step, body, 0)

    def hidden_block(gate_rows, up_rows):
        gate = lax.dot_general(normed[...], gate_rows, NT, preferred_element_type=F32)
        up = lax.dot_general(normed[...], up_rows, NT, preferred_element_type=F32)
        return (gate * jax.nn.sigmoid(gate) * up).astype(BF16)

    def gate_up(c, tasks):
        def body(i, carry):
            slot = lax.rem(c * n_steps + i, 3)
            for copy in load_full(c, i):
                copy.wait()
            pl.when(i + 2 < n_full)(lambda: run(load_full(c, i + 2)))
            pl.when(i + 2 == n_full)(lambda: run(load_rest(c)))
            if c + 1 < CHUNKS:
                pl.when(i + 2 == n_full + 1)(lambda: run(load_full(c + 1, 0)))
            act[:, pl.ds(pl.multiple_of(i * N_BLOCK, N_BLOCK), N_BLOCK)] = hidden_block(gate_w[slot], up_w[slot])
            for at, task in tasks:
                pl.when(i == at)(task)
            return carry

        lax.fori_loop(0, n_full, body, 0)
        for copy in load_rest(c):
            copy.wait()
        if c + 1 < CHUNKS:
            run(load_full(c + 1, 1))
        slot = (c * n_steps + n_full) % 3
        act[:, n_full * N_BLOCK:] = hidden_block(gate_w[slot, :n_rest], up_w[slot, :n_rest])

    def down(c, tasks):
        def body(s, carry):
            for way in range(2):
                jj = c * 2 * ring + 2 * s + way
                load_down(jj).wait()
                pl.when(jj + 2 < CHUNKS * 2 * ring)(lambda: load_down(jj + 2).start())
                part_sum[c, s, way] = jnp.dot(act[...], down_w[lax.rem(jj, 3)], preferred_element_type=F32)

            @pl.when(s == 0)
            def _():
                for sub in range(per_chunk):
                    for way in range(2):
                        rs_send_copy(c * per_chunk + sub, 0, way).start()

            for at, task in tasks:
                pl.when(s == at)(task)
            return carry

        lax.fori_loop(0, ring, body, 0)

    do = functools.partial
    mid_start(0)
    mid_forward(0)
    mid_start(1)
    mid_settle(0)
    normalise(0)
    gate_up(0, [(7, do(mid_forward, 1))])
    down(0, [])
    mid_settle(1)
    normalise(1)
    gate_up(1, [(2, do(rs_step, 0, 1)), (5, do(rs_step, 1, 1)), (8, do(rs_step, 0, 2))])
    down(1, [(0, do(rs_step, 1, 2)), (2, do(rs_final, 0)), (3, do(rs_final, 1))])
    rs_step(2, 1)
    rs_step(3, 1)
    ag_forward(0)
    ag_forward(1)
    rs_step(2, 2)
    rs_step(3, 2)
    ag_settle(0)
    ag_settle(1)
    rs_final(2)
    rs_final(3)
    ag_forward(2)
    ag_forward(3)
    ag_settle(2)
    ag_settle(3)
    for c in range(CHUNKS):
        for way in range(2):
            mid_direct(c, way).wait_send()
            mid_passed(c, way).wait_send()
    for r in range(GROUPS):
        for way in range(2):
            for s in range(ring - 1):
                rs_send_copy(r, s, way).wait_send()
            ag_direct(r, way).wait_send()
            ag_passed(r, way).wait_send()
        for src in range(ring):
            put_out(r, src).wait()


def mlp(call_id, ring, x_mid, gain, w_gate, w_up, w_down):
    tokens, block = x_mid.shape
    hid, width = w_gate.shape
    rows_c, rows_g = tokens // CHUNKS, tokens // GROUPS
    dma = pltpu.SemaphoreType.DMA
    return pl.pallas_call(
        functools.partial(mlp_kernel, ring),
        out_shape=jax.ShapeDtypeStruct((tokens, width), BF16),
        in_specs=[ANY, pl.BlockSpec(memory_space=pltpu.VMEM), ANY, ANY, ANY],
        out_specs=ANY,
        scratch_shapes=[
            pltpu.VMEM((ring, tokens, block), BF16),
            pltpu.VMEM((rows_c, width), BF16),
            pltpu.VMEM((3, N_BLOCK, width), BF16),
            pltpu.VMEM((3, N_BLOCK, width), BF16),
            pltpu.VMEM((rows_c, hid), BF16),
            pltpu.VMEM((3, hid, block // 2), BF16),
            pltpu.VMEM((CHUNKS, ring, 2, rows_c, block // 2), F32),
            pltpu.VMEM((GROUPS, ring - 1, 2, rows_g, block // 2), F32),
            pltpu.VMEM((ring, tokens, block), BF16),
            dma((CHUNKS,)), dma((2, 3)), dma((3,)),
            dma((CHUNKS, 2, 2)), dma((CHUNKS, 2, 2)),
            dma((GROUPS, ring - 1, 2)), dma((GROUPS, ring - 1, 2)),
            dma((GROUPS, 2, 2)), dma((GROUPS, 2, 2)),
            dma((GROUPS, ring)),
        ],
        compiler_params=pltpu.CompilerParams(collective_id=call_id, has_side_effects=True, vmem_limit_bytes=VMEM_MAX),
        cost_estimate=pl.CostEstimate(flops=6 * tokens * width * hid, bytes_accessed=140 * 2**20, transcendentals=tokens * hid),
        name="mlp",
    )(x_mid, gain, w_gate, w_up, w_down)


def solution(mesh):
    owners = mesh.shape["pool"]
    ring = mesh.shape["heads"]
    assert ring == 4 and owners == 8

    def local_fn(kv_pool, page_idx, x_tokens, gain_attn, w_q, w_k, w_v, w_o, gain_mlp, w_gate, w_up, w_down):
        layers, _, _, page_len, kv_loc, head_dim = kv_pool.shape
        tokens = x_tokens.shape[1]
        req_pages = page_idx.shape[2]
        wanted = page_idx.reshape(owners * req_pages)
        cos_tab, sin_tab = rope_tables(owners * req_pages * page_len, tokens, head_dim)
        hidden = x_tokens[0]
        for layer in range(layers):
            picked = pick_pages(kv_pool[layer], wanted, owners)
            x_mid = front(2 * layer, ring, owners, picked, hidden, w_q[layer], w_k[layer], w_v[layer], w_o[layer], gain_attn[layer][None], cos_tab, sin_tab)
            hidden = mlp(2 * layer + 1, ring, x_mid, gain_mlp[layer][None], w_gate[layer].T, w_up[layer].T, w_down[layer])
        return hidden[None]

    pool_spec = P(None, ("rep", "pool"), None, None, "heads", None)
    index_spec = P("rep", "pool", None)
    x_spec = P(("rep", "pool"), None, None)
    gain_spec = P(None, None)
    col_spec = P(None, None, "heads")
    row_spec = P(None, "heads", None)
    return jax.shard_map(local_fn, mesh=mesh, in_specs=(pool_spec, index_spec, x_spec, gain_spec, col_spec, col_spec, col_spec, row_spec, gain_spec, col_spec, col_spec, row_spec), out_specs=x_spec, check_vma=False)
```

```python
import functools

import jax
import jax.numpy as jnp
import numpy as np
from jax import lax
from jax.experimental import pallas as pl
from jax.experimental.pallas import tpu as pltpu
from jax.sharding import PartitionSpec as P

MESH = pl.DeviceIdType.MESH
BF16 = jnp.bfloat16
F32 = jnp.float32
ANY = pl.BlockSpec(memory_space=pl.ANY)
VMEM_MAX = 67043328


def rope_tables(prefix, tokens, head_dim):
    positions = (prefix + np.arange(tokens)).astype(np.float32)
    inv_freq = np.float32(10000.0) ** (-2.0 * np.arange(head_dim // 2).astype(np.float32) / head_dim).astype(np.float32)
    angles = positions[:, None] * inv_freq[None, :]
    cos_half, sin_half = np.cos(angles), np.sin(angles)
    return np.concatenate([cos_half, cos_half], axis=-1), np.concatenate([-sin_half, sin_half], axis=-1)


def pick_kernel(idx_ref, page_ref, out_ref):
    for side in range(2):
        out_ref[0, :, 0, side] = jnp.swapaxes(page_ref[0, side], 0, 1)


def pick_pages(pool, wanted, owners):
    _, _, page_len, heads, head_dim = pool.shape
    each = wanted.shape[0] // owners
    return pl.pallas_call(
        pick_kernel,
        grid_spec=pltpu.PrefetchScalarGridSpec(
            num_scalar_prefetch=1,
            grid=(wanted.shape[0],),
            in_specs=[pl.BlockSpec((1, 2, page_len, heads, head_dim), lambda i, idx: (idx[i], 0, 0, 0, 0))],
            out_specs=pl.BlockSpec((1, heads, 1, 2, page_len, head_dim), lambda i, idx: (i // each, 0, i % each, 0, 0, 0)),
        ),
        out_shape=jax.ShapeDtypeStruct((owners, heads, each, 2, page_len, head_dim), pool.dtype),
        name="pick_pages",
    )(wanted, pool)


NT = (((1,), (1,)), ((), ()))


def remote(src, dst, send_sem, recv_sem, **target):
    return pltpu.make_async_remote_copy(
        src_ref=src, dst_ref=dst, send_sem=send_sem, recv_sem=recv_sem, device_id=target, device_id_type=MESH
    )


def signal_all(targets):
    barrier = pltpu.get_barrier_semaphore()
    for target in targets:
        pl.semaphore_signal(barrier, inc=1, device_id=target, device_id_type=MESH)
    pl.semaphore_wait(barrier, len(targets))


PAIR = 256
SPREAD = 64


def front_kernel(ring, owners, kv_ref, x_ref, wq_ref, wk_ref, wv_ref, wo_ref, gain_ref, cos_ref, sin_ref, mid_ref,
                 x_buf, normed, w_buf, proj, kv_buf, gathered, wo_buf, own_wo, total, mid_buf,
                 local_sem, w_sem, kv_send, kv_recv, a_send, a_recv, wo_send, wo_recv, rest_send, rest_recv):
    me, here = lax.axis_index("heads"), lax.axis_index("pool")
    right, left = lax.rem(me + 1, ring), lax.rem(me + ring - 1, ring)
    tokens, width = x_ref.shape
    heads = kv_buf.shape[1]
    head_dim = kv_buf.shape[-1]
    prefix = owners * kv_buf.shape[2] * kv_buf.shape[4]
    block = width // ring
    half = tokens // 2
    scale = head_dim ** -0.5
    pairs = heads * head_dim // PAIR
    per_pair = PAIR // head_dim
    w_refs = (wq_ref, wk_ref, wv_ref)

    def load_pair(hp):
        cols = pl.ds(pl.multiple_of(hp * PAIR, PAIR), PAIR)
        slot = lax.rem(hp, 2)
        return [pltpu.make_async_copy(w_refs[m].at[:, cols], w_buf.at[slot, m], w_sem.at[slot, m]) for m in range(3)]

    x_copy = pltpu.make_async_copy(x_ref, x_buf, local_sem.at[0])
    x_copy.start()
    kv_own = pltpu.make_async_copy(kv_ref.at[here], kv_buf.at[here], local_sem.at[1])
    kv_own.start()
    for copy in load_pair(0):
        copy.start()
    wo_own = pltpu.make_async_copy(wo_ref.at[:, pl.ds(pl.multiple_of(me * block, block), block)], own_wo, local_sem.at[2])
    wo_own.start()

    signal_all([{"pool": lax.rem(here + t, owners)} for t in range(1, owners)] + [{"heads": lax.rem(me + u, ring)} for u in range(1, ring)])

    piece_rows = wo_ref.shape[0] // owners
    spread_rows = pl.ds(0, SPREAD)
    core = lax.rem(here, 2)
    partner = here + 1 - 2 * core
    chip_right, chip_left = lax.rem(here + 2, owners), lax.rem(here + owners - 2, owners)
    across = lax.rem(here + owners // 2, owners)

    def wo_columns(u, row, rows):
        dest = lax.rem(me + u, ring)
        return dest, wo_ref.at[pl.ds(pl.multiple_of(row, 16), rows), pl.ds(pl.multiple_of(dest * block, block), block)]

    def wo_bring(u):
        dest, src = wo_columns(u, here * piece_rows, SPREAD)
        return remote(src, wo_buf.at[u - 1, here, spread_rows], wo_send.at[u - 1], wo_recv.at[u - 1], heads=dest)

    def wo_spread(i):
        piece = wo_buf.at[:, here, spread_rows]
        return remote(piece, piece, wo_send.at[3 + i], wo_recv.at[3 + i], pool=(chip_right, chip_left, partner)[i])

    def wo_onward(i):
        piece = wo_buf.at[:, (chip_left, chip_right)[i], pl.ds(i * (SPREAD // 2), SPREAD // 2)]
        return remote(piece, piece, wo_send.at[6 + i], wo_recv.at[6 + i], pool=(chip_right, chip_left)[i])

    def wo_beside(i):
        piece = wo_buf.at[:, (chip_left, chip_right)[i], spread_rows]
        return remote(piece, piece, wo_send.at[8 + i], wo_recv.at[8 + i], pool=partner)

    def wo_beside_far(i):
        piece = wo_buf.at[:, across, pl.ds(i * (SPREAD // 2), SPREAD // 2)]
        return remote(piece, piece, wo_send.at[10 + i], wo_recv.at[10 + i], pool=partner)

    rest = piece_rows - SPREAD
    rest_rows = pl.ds(SPREAD, rest)
    chips = owners // 2

    def wo_rest(u, i):
        piece = 2 * i + core
        dest, src = wo_columns(u, piece * piece_rows + SPREAD, rest)
        return remote(src, wo_buf.at[u - 1, piece, rest_rows], rest_send.at[u - 1, i], rest_recv.at[u - 1, i], heads=dest)

    def wo_hand(i):
        piece = wo_buf.at[:, 2 * i + core, rest_rows]
        return remote(piece, piece, rest_send.at[ring - 1, i], rest_recv.at[ring - 1, i], pool=partner)

    for u in range(1, ring):
        wo_bring(u).start()
    def rest_start(i):
        for u in (2, 1, 3):
            wo_rest(u, i).start()

    early = chips // 2
    for i in range(early):
        rest_start(i)

    def page_copy(g, t):
        dest = lax.rem(here + t, owners)
        return remote(kv_ref.at[dest, g], kv_buf.at[here, g], kv_send.at[t - 1, g], kv_recv.at[t - 1, g], pool=dest)

    order = sorted(range(1, owners), key=lambda t: -min(t, owners - t))

    def send_pages(g, carry):
        for t in order:
            page_copy(g, t).start()
        return carry

    lax.fori_loop(0, heads, send_pages, 0)

    x_copy.wait()
    step = 64

    def normalise(i, carry):
        rows = pl.ds(pl.multiple_of(i * step, step), step)
        val = x_buf[rows].astype(F32)
        inv_rms = lax.rsqrt(jnp.mean(val * val, axis=-1, keepdims=True) + 1e-5)
        normed[rows] = (val * inv_rms * gain_ref[...].astype(F32)).astype(BF16)
        return carry

    lax.fori_loop(0, tokens // step, normalise, 0)
    kv_own.wait()

    def all_heads(src):
        return jnp.concatenate([gathered[src, g] for g in range(heads)], axis=-1)

    def a_direct(g, way):
        piece = gathered.at[me, g]
        return remote(piece, piece, a_send.at[g, 0, way], a_recv.at[g, 0, way], heads=(right, left)[way])

    def a_passed(g, way):
        piece = gathered.at[(left, right)[way], g, pl.ds(way * half, half)]
        return remote(piece, piece, a_send.at[g, 1, way], a_recv.at[g, 1, way], heads=(right, left)[way])

    def a_forward(g):
        for way in range(2):
            a_direct(g, way).wait_recv()
            a_passed(g, way).start()

    def rope(val):
        return (val * cos_ref[...] + pltpu.roll(val, head_dim // 2, 1) * sin_ref[...]).astype(BF16)

    def attend(hp, sub):
        g = hp * per_pair + sub
        cols = slice(sub * head_dim, (sub + 1) * head_dim)
        for t in range(1, owners):
            page_copy(g, t).wait_recv()
        keys_pre = kv_buf[:, g, :, 0].reshape(prefix, head_dim)
        vals_pre = kv_buf[:, g, :, 1].reshape(prefix, head_dim)
        for part in range(2):
            rows = slice(part * half, (part + 1) * half)
            seen = (part + 1) * half
            q_part = proj[0, rows, cols]
            s_pre = lax.dot_general(q_part, keys_pre, NT, preferred_element_type=F32) * scale
            s_new = lax.dot_general(q_part, proj[1, :seen, cols], NT, preferred_element_type=F32) * scale
            t_id = lax.broadcasted_iota(jnp.int32, s_new.shape, 0) + part * half
            u_id = lax.broadcasted_iota(jnp.int32, s_new.shape, 1)
            s_new = jnp.where(t_id >= u_id, s_new, -jnp.inf)
            row_max = jnp.maximum(jnp.max(s_pre, axis=-1, keepdims=True), jnp.max(s_new, axis=-1, keepdims=True))
            e_pre = jnp.exp(s_pre - row_max)
            e_new = jnp.exp(s_new - row_max)
            inv_den = 1.0 / (jnp.sum(e_pre, axis=-1, keepdims=True) + jnp.sum(e_new, axis=-1, keepdims=True))
            out = jnp.dot((e_pre * inv_den).astype(BF16), vals_pre, preferred_element_type=F32)
            out = out + jnp.dot((e_new * inv_den).astype(BF16), proj[2, :seen, cols], preferred_element_type=F32)
            gathered[me, g, rows] = out.astype(BF16)
        for way in range(2):
            a_direct(g, way).start()

    def one_pair(hp, carry):
        for copy in load_pair(hp):
            copy.wait()

        @pl.when(hp + 1 < pairs)
        def _():
            for copy in load_pair(hp + 1):
                copy.start()

        slot = lax.rem(hp, 2)
        for m in range(3):
            val = jnp.dot(normed[...], w_buf[slot, m], preferred_element_type=F32)
            for sub in range(per_pair):
                cols = slice(sub * head_dim, (sub + 1) * head_dim)
                proj[m, :, cols] = rope(val[:, cols]) if m < 2 else val[:, cols].astype(BF16)
        for sub in range(per_pair):
            attend(hp, sub)
            g = hp * per_pair + sub

            @pl.when(g >= 3)
            def _():
                a_forward(g - 3)

        for i in range(early, chips):
            pl.when(hp == i - early)(functools.partial(rest_start, i))

        @pl.when(hp == 1)
        def _():
            for u in range(1, ring):
                wo_bring(u).wait_recv()
            for i in range(3):
                wo_spread(i).start()

        return carry

    lax.fori_loop(0, pairs, one_pair, 0)
    wo_own.wait()
    total[...] = jnp.dot(all_heads(me), own_wo[...], preferred_element_type=F32)
    for g in range(heads - 3, heads):
        a_forward(g)
    for i in range(chips):
        for u in range(1, ring):
            wo_rest(u, i).wait_recv()
        wo_hand(i).start()

    for i in range(2):
        wo_spread(i).wait_recv()
        wo_onward(i).start()
        wo_beside(i).start()

    def a_settle(g, carry):
        for way in range(2):
            a_direct(g, way).wait_send()
            a_passed(g, way).wait()
        return carry

    lax.fori_loop(0, heads, a_settle, 0)
    for i in range(2):
        wo_onward(i).wait_recv()
        wo_beside_far(i).start()
    wo_spread(2).wait_recv()
    for i in range(2):
        wo_beside(i).wait_recv()
    for i in range(2):
        wo_beside_far(i).wait_recv()
    for i in range(chips):
        wo_hand(i).wait_recv()

    for n in range(2):
        cols = slice(n * block // 2, (n + 1) * block // 2)
        res = total[:, cols]
        for u in range(1, ring):
            weight = wo_buf[u - 1, :, :, cols].reshape(owners * piece_rows, block // 2)
            res = res + jnp.dot(all_heads(lax.rem(me + ring - u, ring)), weight, preferred_element_type=F32)
        x_cols = pl.ds(pl.multiple_of(me * block + n * (block // 2), block // 2), block // 2)
        mid_buf[:, cols] = (x_buf[:, x_cols].astype(F32) + res).astype(BF16)
    mid_copy = pltpu.make_async_copy(mid_buf, mid_ref, local_sem.at[0])
    mid_copy.start()

    def page_settle(g, carry):
        for t in range(1, owners):
            page_copy(g, t).wait_send()
        return carry

    lax.fori_loop(0, heads, page_settle, 0)
    for u in range(1, ring):
        wo_bring(u).wait_send()
    for i in range(chips):
        for u in range(1, ring):
            wo_rest(u, i).wait_send()
        wo_hand(i).wait_send()
    for i in range(3):
        wo_spread(i).wait_send()
    for i in range(2):
        wo_onward(i).wait_send()
        wo_beside(i).wait_send()
        wo_beside_far(i).wait_send()
    mid_copy.wait()


def front(call_id, ring, owners, kv, x, w_q, w_k, w_v, w_o, gain, cos_tab, sin_tab):
    tokens, width = x.shape
    heads, head_dim = kv.shape[1], kv.shape[-1]
    block = width // ring
    local = heads * head_dim
    dma = pltpu.SemaphoreType.DMA
    in_vmem = pl.BlockSpec(memory_space=pltpu.VMEM)
    return pl.pallas_call(
        functools.partial(front_kernel, ring, owners),
        out_shape=jax.ShapeDtypeStruct((tokens, block), BF16),
        in_specs=[ANY] * 6 + [in_vmem] * 3,
        out_specs=ANY,
        scratch_shapes=[
            pltpu.VMEM((tokens, width), BF16),
            pltpu.VMEM((tokens, width), BF16),
            pltpu.VMEM((2, 3, width, PAIR), BF16),
            pltpu.VMEM((3, tokens, PAIR), BF16),
            pltpu.VMEM(kv.shape, BF16),
            pltpu.VMEM((ring, heads, tokens, head_dim), BF16),
            pltpu.VMEM((ring - 1, owners, local // owners, block), BF16),
            pltpu.VMEM((local, block), BF16),
            pltpu.VMEM((tokens, block), F32),
            pltpu.VMEM((tokens, block), BF16),
            dma((3,)), dma((2, 3)),
            dma((owners - 1, heads)), dma((owners - 1, heads)),
            dma((heads, 2, 2)), dma((heads, 2, 2)),
            dma((12,)), dma((12,)),
            dma((ring, owners // 2)), dma((ring, owners // 2)),
        ],
        compiler_params=pltpu.CompilerParams(collective_id=call_id, has_side_effects=True, vmem_limit_bytes=VMEM_MAX),
        cost_estimate=pl.CostEstimate(flops=8 * tokens * width * local, bytes_accessed=48 * 2**20, transcendentals=heads * tokens * 3 * tokens),
        name="front",
    )(kv, x, w_q, w_k, w_v, w_o, gain, cos_tab, sin_tab)


CHUNKS = 2
GROUPS = 4
N_BLOCK = 256


def mlp_kernel(ring, x_ref, gain_ref, wg_ref, wu_ref, wd_ref, out_ref,
               mid, normed, gate_w, up_w, act, down_w, part_sum, running, result,
               local_sem, w_sem, d_sem, mid_send, mid_recv, rs_send, rs_recv, ag_send, ag_recv, out_sem):
    me = lax.axis_index("heads")
    right, left = lax.rem(me + 1, ring), lax.rem(me + ring - 1, ring)
    ways = (right, left)
    tokens, block = x_ref.shape
    width = block * ring
    hid = wg_ref.shape[0]
    rows_c = tokens // CHUNKS
    rows_g = tokens // GROUPS
    per_chunk = GROUPS // CHUNKS
    n_half = block // 2
    n_full, n_rest = hid // N_BLOCK, hid % N_BLOCK
    n_steps = n_full + 1

    x_copies = []
    for c in range(CHUNKS):
        rows = pl.ds(c * rows_c, rows_c)
        x_copies.append(pltpu.make_async_copy(x_ref.at[rows], mid.at[me, rows], local_sem.at[c]))
        x_copies[c].start()

    def load_full(c, i):
        rows = pl.ds(pl.multiple_of(i * N_BLOCK, N_BLOCK), N_BLOCK)
        slot = lax.rem(c * n_steps + i, 3)
        return (pltpu.make_async_copy(wg_ref.at[rows], gate_w.at[slot], w_sem.at[0, slot]),
                pltpu.make_async_copy(wu_ref.at[rows], up_w.at[slot], w_sem.at[1, slot]))

    def load_rest(c):
        rows, dst = pl.ds(n_full * N_BLOCK, n_rest), pl.ds(0, n_rest)
        slot = (c * n_steps + n_full) % 3
        return (pltpu.make_async_copy(wg_ref.at[rows], gate_w.at[slot, dst], w_sem.at[0, slot]),
                pltpu.make_async_copy(wu_ref.at[rows], up_w.at[slot, dst], w_sem.at[1, slot]))

    def run(copies):
        for copy in copies:
            copy.start()

    def load_down(jj):
        s, way = lax.rem(jj // 2, ring), lax.rem(jj, 2)
        blk = jnp.where(way == 0, lax.rem(me + 2 * ring - 1 - s, ring), lax.rem(me + 1 + s, ring))
        col = pl.multiple_of(blk * block + way * n_half, n_half)
        slot = lax.rem(jj, 3)
        return pltpu.make_async_copy(wd_ref.at[:, pl.ds(col, n_half)], down_w.at[slot], d_sem.at[slot])

    signal_all([{"heads": right}, {"heads": left}])

    def mid_direct(c, way):
        piece = mid.at[me, pl.ds(c * rows_c, rows_c)]
        return remote(piece, piece, mid_send.at[c, 0, way], mid_recv.at[c, 0, way], heads=ways[way])

    def mid_passed(c, way):
        piece = mid.at[(left, right)[way], pl.ds(c * rows_c + way * (rows_c // 2), rows_c // 2)]
        return remote(piece, piece, mid_send.at[c, 1, way], mid_recv.at[c, 1, way], heads=ways[way])

    def mid_start(c):
        x_copies[c].wait()
        for way in range(2):
            mid_direct(c, way).start()

    def mid_forward(c):
        for way in range(2):
            mid_direct(c, way).wait_recv()
            mid_passed(c, way).start()

    def mid_settle(c):
        for way in range(2):
            mid_passed(c, way).wait_recv()

    def rs_send_copy(r, s, way):
        rows = pl.ds((r % per_chunk) * rows_g, rows_g)
        src = part_sum.at[r // per_chunk, 0, way, rows] if s == 0 else running.at[r, s - 1, way]
        return remote(src, running.at[r, s, way], rs_send.at[r, s, way], rs_recv.at[r, s, way], heads=ways[way])

    def rs_step(r, s):
        rows = slice((r % per_chunk) * rows_g, (r % per_chunk + 1) * rows_g)
        for way in range(2):
            rs_send_copy(r, s - 1, way).wait_recv()
            running[r, s - 1, way] = running[r, s - 1, way] + part_sum[r // per_chunk, s, way, rows]
            rs_send_copy(r, s, way).start()

    def ag_direct(r, way):
        piece = result.at[me, pl.ds(r * rows_g, rows_g)]
        return remote(piece, piece, ag_send.at[r, 0, way], ag_recv.at[r, 0, way], heads=ways[way])

    def ag_passed(r, way):
        piece = result.at[(left, right)[way], pl.ds(r * rows_g + way * (rows_g // 2), rows_g // 2)]
        return remote(piece, piece, ag_send.at[r, 1, way], ag_recv.at[r, 1, way], heads=ways[way])

    def rs_final(r):
        rows = slice((r % per_chunk) * rows_g, (r % per_chunk + 1) * rows_g)
        dst = slice(r * rows_g, (r + 1) * rows_g)
        for way in range(2):
            rs_send_copy(r, ring - 2, way).wait_recv()
            cols = slice(way * n_half, (way + 1) * n_half)
            total = running[r, ring - 2, way] + part_sum[r // per_chunk, ring - 1, way, rows]
            result[me, dst, cols] = (mid[me, dst, cols].astype(F32) + total).astype(BF16)
        for way in range(2):
            ag_direct(r, way).start()

    def ag_forward(r):
        for way in range(2):
            ag_direct(r, way).wait_recv()
            ag_passed(r, way).start()

    def put_out(r, src):
        rows = pl.ds(r * rows_g, rows_g)
        return pltpu.make_async_copy(result.at[src, rows], out_ref.at[rows, pl.ds(src * block, block)], out_sem.at[r, src])

    def ag_settle(r):
        for way in range(2):
            ag_passed(r, way).wait_recv()
        for src in range(ring):
            put_out(r, src).start()

    def normalise(c):
        step = 64

        def body(i, carry):
            base = pl.multiple_of(i * step, step)
            rows, out_rows = pl.ds(c * rows_c + base, step), pl.ds(base, step)
            squares = jnp.zeros((step, 1), F32)
            for b in range(ring):
                val = mid[b, rows].astype(F32)
                squares = squares + jnp.sum(val * val, axis=-1, keepdims=True)
            inv_rms = lax.rsqrt(squares * (1.0 / width) + 1e-5)
            for b in range(ring):
                cols = slice(b * block, (b + 1) * block)
                normed[out_rows, cols] = (mid[b, rows].astype(F32) * inv_rms * gain_ref[:, cols].astype(F32)).astype(BF16)
            return carry

        lax.fori_loop(0, rows_c // step, body, 0)

    def hidden_block(gate_rows, up_rows):
        gate = lax.dot_general(normed[...], gate_rows, NT, preferred_element_type=F32)
        up = lax.dot_general(normed[...], up_rows, NT, preferred_element_type=F32)
        return (gate * jax.nn.sigmoid(gate) * up).astype(BF16)

    def gate_up(c, tasks):
        def body(i, carry):
            slot = lax.rem(c * n_steps + i, 3)
            for copy in load_full(c, i):
                copy.wait()
            pl.when(i + 2 < n_full)(lambda: run(load_full(c, i + 2)))
            pl.when(i + 2 == n_full)(lambda: run(load_rest(c)))
            if c + 1 < CHUNKS:
                pl.when(i + 2 == n_full + 1)(lambda: run(load_full(c + 1, 0)))
            act[:, pl.ds(pl.multiple_of(i * N_BLOCK, N_BLOCK), N_BLOCK)] = hidden_block(gate_w[slot], up_w[slot])
            for at, task in tasks:
                pl.when(i == at)(task)
            return carry

        lax.fori_loop(0, n_full, body, 0)
        for copy in load_rest(c):
            copy.wait()
        if c + 1 < CHUNKS:
            run(load_full(c + 1, 1))
        slot = (c * n_steps + n_full) % 3
        act[:, n_full * N_BLOCK:] = hidden_block(gate_w[slot, :n_rest], up_w[slot, :n_rest])

    def down(c, tasks):
        def body(s, carry):
            for way in range(2):
                jj = c * 2 * ring + 2 * s + way
                load_down(jj).wait()
                pl.when(jj + 2 < CHUNKS * 2 * ring)(lambda: load_down(jj + 2).start())
                part_sum[c, s, way] = jnp.dot(act[...], down_w[lax.rem(jj, 3)], preferred_element_type=F32)

            @pl.when(s == 0)
            def _():
                for sub in range(per_chunk):
                    for way in range(2):
                        rs_send_copy(c * per_chunk + sub, 0, way).start()

            for at, task in tasks:
                pl.when(s == at)(task)
            return carry

        lax.fori_loop(0, ring, body, 0)

    do = functools.partial
    mid_start(0)
    run(load_full(0, 0))
    run(load_full(0, 1))
    for jj in range(2):
        load_down(jj).start()
    mid_forward(0)
    mid_start(1)
    mid_settle(0)
    normalise(0)
    gate_up(0, [(7, do(mid_forward, 1))])
    down(0, [])
    mid_settle(1)
    normalise(1)
    gate_up(1, [(2, do(rs_step, 0, 1)), (5, do(rs_step, 1, 1)), (8, do(rs_step, 0, 2))])
    down(1, [(0, do(rs_step, 1, 2)), (2, do(rs_final, 0)), (3, do(rs_final, 1))])
    rs_step(2, 1)
    rs_step(3, 1)
    ag_forward(0)
    ag_forward(1)
    rs_step(2, 2)
    rs_step(3, 2)
    ag_settle(0)
    ag_settle(1)
    rs_final(2)
    rs_final(3)
    ag_forward(2)
    ag_forward(3)
    ag_settle(2)
    ag_settle(3)
    for c in range(CHUNKS):
        for way in range(2):
            mid_direct(c, way).wait_send()
            mid_passed(c, way).wait_send()
    for r in range(GROUPS):
        for way in range(2):
            for s in range(ring - 1):
                rs_send_copy(r, s, way).wait_send()
            ag_direct(r, way).wait_send()
            ag_passed(r, way).wait_send()
        for src in range(ring):
            put_out(r, src).wait()


def mlp(call_id, ring, x_mid, gain, w_gate, w_up, w_down):
    tokens, block = x_mid.shape
    hid, width = w_gate.shape
    rows_c, rows_g = tokens // CHUNKS, tokens // GROUPS
    dma = pltpu.SemaphoreType.DMA
    return pl.pallas_call(
        functools.partial(mlp_kernel, ring),
        out_shape=jax.ShapeDtypeStruct((tokens, width), BF16),
        in_specs=[ANY, pl.BlockSpec(memory_space=pltpu.VMEM), ANY, ANY, ANY],
        out_specs=ANY,
        scratch_shapes=[
            pltpu.VMEM((ring, tokens, block), BF16),
            pltpu.VMEM((rows_c, width), BF16),
            pltpu.VMEM((3, N_BLOCK, width), BF16),
            pltpu.VMEM((3, N_BLOCK, width), BF16),
            pltpu.VMEM((rows_c, hid), BF16),
            pltpu.VMEM((3, hid, block // 2), BF16),
            pltpu.VMEM((CHUNKS, ring, 2, rows_c, block // 2), F32),
            pltpu.VMEM((GROUPS, ring - 1, 2, rows_g, block // 2), F32),
            pltpu.VMEM((ring, tokens, block), BF16),
            dma((CHUNKS,)), dma((2, 3)), dma((3,)),
            dma((CHUNKS, 2, 2)), dma((CHUNKS, 2, 2)),
            dma((GROUPS, ring - 1, 2)), dma((GROUPS, ring - 1, 2)),
            dma((GROUPS, 2, 2)), dma((GROUPS, 2, 2)),
            dma((GROUPS, ring)),
        ],
        compiler_params=pltpu.CompilerParams(collective_id=call_id, has_side_effects=True, vmem_limit_bytes=VMEM_MAX),
        cost_estimate=pl.CostEstimate(flops=6 * tokens * width * hid, bytes_accessed=140 * 2**20, transcendentals=tokens * hid),
        name="mlp",
    )(x_mid, gain, w_gate, w_up, w_down)


def solution(mesh):
    owners = mesh.shape["pool"]
    ring = mesh.shape["heads"]
    assert ring == 4 and owners == 8

    def local_fn(kv_pool, page_idx, x_tokens, gain_attn, w_q, w_k, w_v, w_o, gain_mlp, w_gate, w_up, w_down):
        layers, _, _, page_len, kv_loc, head_dim = kv_pool.shape
        tokens = x_tokens.shape[1]
        req_pages = page_idx.shape[2]
        wanted = page_idx.reshape(owners * req_pages)
        cos_tab, sin_tab = rope_tables(owners * req_pages * page_len, tokens, head_dim)
        hidden = x_tokens[0]
        for layer in range(layers):
            picked = pick_pages(kv_pool[layer], wanted, owners)
            x_mid = front(2 * layer, ring, owners, picked, hidden, w_q[layer], w_k[layer], w_v[layer], w_o[layer], gain_attn[layer][None], cos_tab, sin_tab)
            hidden = mlp(2 * layer + 1, ring, x_mid, gain_mlp[layer][None], w_gate[layer].T, w_up[layer].T, w_down[layer])
        return hidden[None]

    pool_spec = P(None, ("rep", "pool"), None, None, "heads", None)
    index_spec = P("rep", "pool", None)
    x_spec = P(("rep", "pool"), None, None)
    gain_spec = P(None, None)
    col_spec = P(None, None, "heads")
    row_spec = P(None, "heads", None)
    return jax.shard_map(local_fn, mesh=mesh, in_specs=(pool_spec, index_spec, x_spec, gain_spec, col_spec, col_spec, col_spec, row_spec, gain_spec, col_spec, col_spec, row_spec), out_specs=x_spec, check_vma=False)
```
